32 devices in a mesh: rep: 2 (over y), seq: 4 (over z), section: 2 (over core), head: 2 (over x).
Axes of the slice: x: 2, y: 2, z: 4, core: 2. Of those that a mesh axis runs over, the one named last changes fastest.
Arguments:
- hidden: bfloat16 [6, 256, 2048], P('rep', 'seq'), parts along dimension 0, may hold values from -6 to 6
- lengths: int32 [6], P('rep'), parts along dimension 0, may hold values from 1 to 256, 576 in all
- attn_gain: float32 [2, 2048], P('section'), may hold values from 0.1 to 1.9
- w_query: bfloat16 [2, 2048, 2048], P('section', None, 'head'), may hold values from -2 to 2
- w_latent: bfloat16 [2, 2048, 512], P('section'), may hold values from -0.125 to 0.125
- latent_gain: float32 [2, 512], P('section'), may hold values from 0.1 to 1.9
- w_key: bfloat16 [2, 512, 2048], P('section', None, 'head'), may hold values from -0.25 to 0.25
- w_value: bfloat16 [2, 512, 2048], P('section', None, 'head'), may hold values from -0.25 to 0.25
- w_out: bfloat16 [2, 2048, 2048], P('section', 'head'), may hold values from -0.125 to 0.125
Outputs:
- final: float32 [6, 256, 2048], P('rep', ('seq', 'head'), 'section'), parts along dimension 0
- latents: float32 [2, 6, 256, 512], P('section', 'rep', 'seq'), parts along dimension 1
The draws below stay inside these ranges and needn't reach their ends.
There are 2 independent parts, one for each index of `rep`. The reference program is written for one: setup_inputs(seed, part) draws one part's arguments, and reference() takes and returns one part's arrays. A program takes and returns all parts, laid end to end along the dimension named above; an argument that names none is the same for every part. Nothing has to cross between parts.
Inputs may be any that keep to these rules, and one draw needn't show every extreme that they name: lengths sum to 576 and one block holds exactly 256; the live tokens of a block are its first slots.
All inputs are finite; a program needn't handle non-finite values.
Results may differ from the reference program's by a relative error of at most 0.015.
The reference program's roundings to bfloat16 on the way (of `normed`, `query`, `latent`, `absorbed`, `rounded`, `context` and `attn`) count: a program that leaves them out, or rounds other values in their place, can miss the bound.
Values may be sent and summed in bfloat16 or wider, within the bound.
No kernel may reach another device: no remote copies, remote signals or barrier semaphores. Data moves between devices by JAX's collectives and lax.ppermute only.
A program may use at most 128 MiB of HBM per device.

```python
import math
import jax
import jax.numpy as jnp
import numpy as np
from jax import lax

D = 2048
HEADS = 16
HD = 128
R = 512
GROUPS = 3
TOKC = 256
LAYERS = 2


def draw_w_query(key, part):
    full_shape = (LAYERS, D, HEADS * HD)
    entries = jax.random.truncated_normal(key, -6.0, 6.0, full_shape, jnp.float32) * D ** (-0.5)
    return entries.astype(jnp.bfloat16)


def block_levels(stream_key, dims, cuts, smallest, top_value):
    factor_of = 1.0
    for axis_at, parts in cuts:
        draws = jax.random.uniform(jax.random.fold_in(jax.random.fold_in(stream_key, 6), axis_at), (parts,), jnp.float32, smallest / len(cuts), top_value / len(cuts))
        factor_of = factor_of * jnp.repeat(jnp.exp(draws), dims[axis_at] // parts).reshape((-1,) + (1,) * (len(dims) - 1 - axis_at))
    return factor_of


def length_profile(count, total, most, lean):
    loads = [(1 << 20) // math.isqrt(rank ** lean) + 1 for rank in range(2, count + 1)]
    spare, counts = total - most - (count - 1), [1] * (count - 1)
    while spare > 0:
        candidates = [i for i in range(count - 1) if counts[i] < most]
        pool, left = sum([loads[i] for i in candidates]), spare
        for i in candidates:
            more = min(most - counts[i], max(1, left * loads[i] // pool), spare)
            counts[i] = counts[i] + more
            spare = spare - more
    return np.array([most] + counts)


def uneven_parts(stream_key, number_of, total, bound, slope):
    if number_of == 2:
        one = jax.random.randint(stream_key, (), max(1, total - bound), min(bound, total - 1) + 1)
        return jnp.stack([one, total - one])
    tallies = jnp.asarray(length_profile(number_of, total, bound, slope), jnp.int32)
    twos = (number_of - 1) // 2
    source_of, receiver = tallies[1:1 + 2 * twos:2], tallies[2:2 + 2 * twos:2]
    slack = jnp.minimum(source_of - 1, bound - receiver)
    shifted = jax.random.randint(jax.random.fold_in(stream_key, 1), (twos,), 0, 1 << 20) % (slack + 1)
    tallies = tallies.at[1:1 + 2 * twos:2].set(source_of - shifted).at[2:2 + 2 * twos:2].set(receiver + shifted)
    return tallies[jax.random.permutation(jax.random.fold_in(stream_key, 2), number_of)]


def bell_draw(rng, extent, scale, bound, cuts=(), kind=jnp.bfloat16):
    values = scale * jax.random.normal(rng, extent, jnp.float32)
    if cuts:
        values = values * block_levels(rng, extent, cuts, -0.22, 0.18)
    return jnp.clip(values, -bound, bound).astype(kind)


def setup_inputs(seed: int = 0, part: int = 0) -> dict:
    streams_of = jax.random.split(jax.random.key(seed), 10)
    part_splits = jax.random.split(jax.random.fold_in(streams_of[9], part), 10)
    return {
        "hidden": bell_draw(part_splits[0], (GROUPS, TOKC, D), 1.0, 6.0, ((1, 4),)),
        "lengths": uneven_parts(part_splits[1], GROUPS, 3 * GROUPS * TOKC // 4, TOKC, 2).astype(jnp.int32),
        "attn_gain": jnp.clip(1.0 + 0.18 * jax.random.normal(streams_of[2], (LAYERS, D), jnp.float32), 0.1, 1.9),
        "w_query": draw_w_query(jax.random.fold_in(streams_of[9], 71), part),
        "w_latent": bell_draw(streams_of[4], (LAYERS, D, R), D ** -0.5, 0.125, ((0, 2),)),
        "latent_gain": jnp.clip(1.0 + 0.18 * jax.random.normal(streams_of[5], (LAYERS, R), jnp.float32), 0.1, 1.9),
        "w_key": bell_draw(streams_of[6], (LAYERS, R, HEADS * HD), R ** -0.5, 0.25, ((0, 2), (2, 2))),
        "w_value": bell_draw(streams_of[7], (LAYERS, R, HEADS * HD), R ** -0.5, 0.25, ((0, 2), (2, 2))),
        "w_out": bell_draw(streams_of[8], (LAYERS, HEADS * HD, D), (HEADS * HD) ** -0.5, 0.125, ((0, 2), (1, 2))),
    }


def rms_scale(values, gain):
    values = values.astype(jnp.float32)
    mean_sq = lax.optimization_barrier(jnp.mean(values * values, axis=-1, keepdims=True))
    return values * lax.rsqrt(mean_sq + 1e-06) * gain

def reference(hidden, lengths, attn_gain, w_query, w_latent, latent_gain, w_key, w_value, w_out):
    groups, group_rows, width = hidden.shape
    heads = w_key.shape[2] // HD
    rank = w_latent.shape[2]
    position = jnp.arange(group_rows, dtype=jnp.int32)
    block_ids = jnp.arange(groups, dtype=jnp.int32)
    live = position[None, :] < lengths[:, None]
    scale = 1.0 / HD ** 0.5
    state = hidden.astype(jnp.float32)
    stored = []
    for layer in range(LAYERS):
        normed = rms_scale(state, attn_gain[layer]).astype(jnp.bfloat16)
        flat = normed.reshape(groups * group_rows, width)
        query = jnp.dot(flat, w_query[layer], preferred_element_type=jnp.float32).astype(jnp.bfloat16)
        query = query.reshape(groups, group_rows, heads, HD)
        raw = jnp.dot(flat, w_latent[layer], preferred_element_type=jnp.float32)
        latent_full = rms_scale(raw, latent_gain[layer]).reshape(groups, group_rows, rank)
        latent = latent_full.astype(jnp.bfloat16)
        key_map = w_key[layer].astype(jnp.float32).reshape(rank, heads, HD)
        value_map = w_value[layer].astype(jnp.float32).reshape(rank, heads, HD)
        latent_wide = lax.optimization_barrier(latent).astype(jnp.float32)
        pieces = []
        for group in range(groups):
            seen = group + 1
            absorbed = (jnp.einsum('qhd,rhd->hqr', query[group].astype(jnp.float32), key_map) * scale).astype(jnp.bfloat16)
            absorbed_wide = lax.optimization_barrier(absorbed).astype(jnp.float32)
            keys_seen = latent_wide[:seen]
            scores = jnp.einsum('hqr,ckr->hqck', absorbed_wide, keys_seen)
            ids = block_ids[:seen]
            past = (ids < group)[:, None] & live[:seen]
            same = (ids == group)[None, :, None] & (position[None, None, :] <= position[:, None, None])
            mask = past[None] | same
            scores = jnp.where(mask[None], scores, -1e+30)
            top = lax.optimization_barrier(jnp.max(scores, axis=(2, 3), keepdims=True))
            weights = jnp.where(mask[None], jnp.exp(scores - top), 0.0)
            total = lax.optimization_barrier(jnp.sum(weights, axis=(2, 3)))
            rounded = lax.optimization_barrier(weights.astype(jnp.bfloat16)).astype(jnp.float32)
            context = jnp.einsum('hqck,ckr->hqr', rounded, keys_seen) / total[:, :, None]
            context = lax.optimization_barrier(context.astype(jnp.bfloat16)).astype(jnp.float32)
            attn = jnp.einsum('hqr,rhd->qhd', context, value_map)
            pieces.append(attn.reshape(group_rows, heads * HD).astype(jnp.bfloat16))
        attn_all = jnp.concatenate(pieces, axis=0)
        update = jnp.dot(attn_all, w_out[layer], preferred_element_type=jnp.float32)
        state = state + update.reshape(groups, group_rows, width)
        stored.append(jnp.where(live[:, :, None], latent_full, jnp.zeros_like(latent_full)))
    final = jnp.where(live[:, :, None], state, jnp.zeros_like(state))
    return (final, jnp.stack(stored, axis=0))
```

```python
import functools

import jax
import jax.numpy as jnp
from jax import lax
from jax.experimental import pallas as pl
from jax.experimental.pallas import tpu as pltpu
from jax.sharding import PartitionSpec as P

HD = 128
AXES = ("seq", "section", "head")
F32 = jnp.float32
BF16 = jnp.bfloat16
VMEM = pl.BlockSpec(memory_space=pltpu.VMEM)
SMEM = pl.BlockSpec(memory_space=pltpu.SMEM)
MIB = 1 << 20


def permute(value, sizes, target):
    pairs = []
    for s in range(sizes[0]):
        for c in range(sizes[1]):
            for h in range(sizes[2]):
                ts, tc, th = target(s, c, h)
                at = (s * sizes[1] + c) * sizes[2] + h
                to = (ts * sizes[1] + tc) * sizes[2] + th
                pairs.append((at, to))
    return lax.ppermute(value, AXES, pairs)


def rms(values, gain):
    mean_sq = jnp.mean(values * values, axis=-1, keepdims=True)
    return values * lax.rsqrt(mean_sq + 1e-06) * gain


def dot(a, b, dims=((1,), (0,))):
    return lax.dot_general(a, b, (dims, ((), ())), preferred_element_type=F32)


def tree_sum(terms):
    terms = [t.astype(F32) for t in terms]
    while len(terms) > 1:
        terms = [sum(terms[i : i + 2]) for i in range(0, len(terms), 2)]
    return terms[0]


def latent_body(n_parts, *refs):
    x_ref = refs[0]
    parts = refs[1 : 1 + n_parts]
    gain_ref, w_ref, lgain_ref, normed_ref, full_ref, latent_ref = refs[1 + n_parts :]
    state = x_ref[...].astype(F32)
    if n_parts:
        state = state + tree_sum([p[...] for p in parts])
    normed = rms(state, gain_ref[...]).astype(BF16)
    normed_ref[...] = normed
    full = rms(dot(normed, w_ref[...]), lgain_ref[...])
    full_ref[...] = full
    latent_ref[...] = full.astype(BF16)


def query_body(scale, normed_ref, wq_ref, wk_ref, out_ref):
    heads = out_ref.shape[0]
    query = dot(normed_ref[...], wq_ref[...]).astype(BF16)
    for h in range(heads):
        cols = slice(h * HD, (h + 1) * HD)
        one = dot(query[:, cols], wk_ref[:, cols], ((1,), (1,)))
        out_ref[h] = (one * scale).astype(BF16)


def attend_body(groups, rows, n_pieces, *refs):
    seq_ref, lengths_ref, absorbed_ref = refs[:3]
    pieces = refs[3 : 3 + n_pieces]
    wv_ref, wo_ref, out_ref, kv, attn = refs[3 + n_pieces :]
    heads = absorbed_ref.shape[0]
    rank = kv.shape[1]
    block = n_pieces * rows
    me = seq_ref[0]
    for g in range(groups):
        for k in range(n_pieces):
            kv[pl.ds(g * block + k * rows, rows), :] = pieces[k][pl.ds(g * rows, rows), :]
    col = lax.broadcasted_iota(jnp.int32, (rows, block), 1)
    row = lax.broadcasted_iota(jnp.int32, (rows, block), 0)
    key_pos = jnp.bitwise_xor(me, col // rows) * rows + col % rows
    query_pos = me * rows + row
    causal = key_pos <= query_pos
    for g in range(groups):
        keys = kv[: (g + 1) * block, :]
        absorbed = absorbed_ref[:, g * rows : (g + 1) * rows, :].reshape(heads * rows, rank)
        scores = dot(absorbed, keys, ((1,), (1,)))
        mask = [key_pos < lengths_ref[b] for b in range(g)] + [causal]
        mask = jnp.concatenate(mask, axis=1)[None]
        scores = scores.reshape(heads, rows, (g + 1) * block)
        scores = jnp.where(mask, scores, -1e30)
        top = jnp.max(scores, axis=2, keepdims=True)
        weights = jnp.where(mask, jnp.exp(scores - top), 0.0)
        total = jnp.sum(weights, axis=2, keepdims=True).reshape(heads * rows, 1)
        rounded = weights.astype(BF16).reshape(heads * rows, (g + 1) * block)
        context = (dot(rounded, keys) / total).astype(BF16)
        for h in range(heads):
            cols = slice(h * HD, (h + 1) * HD)
            one = dot(context[h * rows : (h + 1) * rows], wv_ref[:, cols])
            attn[g * rows : (g + 1) * rows, cols] = one.astype(BF16)
    out_ref[...] = dot(attn[...], wo_ref[...]).astype(BF16)


def params(limit):
    return pltpu.CompilerParams(vmem_limit_bytes=limit * MIB)


def shards(hidden, lengths, attn_gain, w_query, w_latent, latent_gain, w_key, w_value, w_out):
    n_seq = lax.axis_size("seq")
    n_sec = lax.axis_size("section")
    n_head = lax.axis_size("head")
    sizes = (n_seq, n_sec, n_head)
    seq_id = lax.axis_index("seq")
    section_id = lax.axis_index("section")
    head_id = lax.axis_index("head")
    groups, rows, width = hidden.shape
    rank = w_latent.shape[2]
    heads = w_key.shape[2] // HD
    total_rows = groups * rows
    share = rows // n_head
    part_width = width // n_sec
    x = hidden.reshape(total_rows, width)
    seq_arr = seq_id.astype(jnp.int32).reshape(1)
    wq, wl, wk, wv, wo = w_query[0], w_latent[0], w_key[0], w_value[0], w_out[0]
    latents = []
    parts = []
    for tick in range(n_sec):
        normed, full, latent = pl.pallas_call(
            functools.partial(latent_body, len(parts)),
            out_shape=(
                jax.ShapeDtypeStruct((total_rows, width), BF16),
                jax.ShapeDtypeStruct((total_rows, rank), F32),
                jax.ShapeDtypeStruct((total_rows, rank), BF16),
            ),
            in_specs=[VMEM] * (4 + len(parts)),
            out_specs=(VMEM, VMEM, VMEM),
            compiler_params=params(16),
            cost_estimate=pl.CostEstimate(
                flops=2 * total_rows * width * rank,
                bytes_accessed=2 * width * (rank + 2 * total_rows),
                transcendentals=0,
            ),
            name=f"latent{tick}",
        )(x, *parts, attn_gain, wl, latent_gain)
        latents.append(full)
        pieces = [latent] + [
            permute(latent, sizes, lambda s, c, h, k=k: (s ^ k, c, h) if c == tick else (s, c, h))
            for k in range(1, n_seq)
        ]
        absorbed = pl.pallas_call(
            functools.partial(query_body, 1.0 / HD**0.5),
            out_shape=jax.ShapeDtypeStruct((heads, total_rows, rank), BF16),
            in_specs=[VMEM] * 3,
            out_specs=VMEM,
            compiler_params=params(16),
            cost_estimate=pl.CostEstimate(
                flops=2 * total_rows * heads * HD * (width + rank),
                bytes_accessed=2 * heads * HD * (width + rank + total_rows),
                transcendentals=0,
            ),
            name=f"query{tick}",
        )(normed, wq, wk)
        partial = pl.pallas_call(
            functools.partial(attend_body, groups, rows, n_seq),
            out_shape=jax.ShapeDtypeStruct((total_rows, width), BF16),
            in_specs=[SMEM, SMEM] + [VMEM] * (3 + n_seq),
            out_specs=VMEM,
            scratch_shapes=[
                pltpu.VMEM((groups * n_seq * rows, rank), BF16),
                pltpu.VMEM((total_rows, heads * HD), BF16),
            ],
            compiler_params=params(32),
            cost_estimate=pl.CostEstimate(
                flops=4 * heads * total_rows * groups * n_seq * rows * rank,
                bytes_accessed=2 * heads * HD * (width + rank),
                transcendentals=heads * total_rows * groups * n_seq * rows,
            ),
            name=f"attend{tick}",
        )(seq_arr, lengths, absorbed, *pieces, wv, wo)
        if tick + 1 < n_sec:
            parts = [permute(partial, sizes, lambda s, c, h: (s, (c + 1) % n_sec, h))] + [
                permute(
                    partial,
                    sizes,
                    lambda s, c, h, k=k: (s, c + 1, h ^ k) if c + 1 < n_sec else (s, 0, h),
                )
                for k in range(1, n_head)
            ]
    state = x.astype(F32) + tree_sum(parts)
    mine = partial.reshape(groups, n_head, share, width)
    base = state.reshape(groups, n_head, share, width)
    is_mine = (jnp.arange(n_head) == head_id)[None, :, None, None]
    both = jnp.where(is_mine, base + mine.astype(F32), mine.astype(F32))
    left = both[..., :part_width].astype(BF16)
    came = permute(left, sizes, lambda s, c, h: (s, (c + 1) % n_sec, h))
    half = jnp.where(section_id == n_sec - 1, both[..., part_width:], came.astype(F32))
    own = lax.dynamic_index_in_dim(half, head_id, 1, keepdims=False)
    others = [
        permute(
            lax.dynamic_index_in_dim(half, head_id ^ k, 1, keepdims=False).astype(BF16),
            sizes,
            lambda s, c, h, k=k: (s, c, h ^ k),
        ).astype(F32)
        for k in range(1, n_head)
    ]
    final = sum(others, own)
    out_pos = seq_id * rows + head_id * share + jnp.arange(share, dtype=jnp.int32)
    final = jnp.where((out_pos[None, :] < lengths[:, None])[:, :, None], final, 0.0)
    stored = latents[0]
    for tick in range(1, n_sec):
        stored = jnp.where(section_id == tick, latents[tick], stored)
    query_pos = seq_id * rows + jnp.arange(rows, dtype=jnp.int32)
    live = query_pos[None, :] < lengths[:, None]
    stored = jnp.where(live[..., None], stored.reshape(groups, rows, rank), 0.0)[None]
    return (final, stored)


def solution(mesh):
    return jax.shard_map(
        shards,
        mesh=mesh,
        in_specs=(
            P("rep", "seq", None),
            P("rep"),
            P("section", None),
            P("section", None, "head"),
            P("section", None, None),
            P("section", None),
            P("section", None, "head"),
            P("section", None, "head"),
            P("section", "head", None),
        ),
        out_specs=(P("rep", ("seq", "head"), "section"), P("section", "rep", "seq", None)),
        check_vma=False,
    )
```

```python
import functools

import jax
import jax.numpy as jnp
from jax import lax
from jax.experimental import pallas as pl
from jax.experimental.pallas import tpu as pltpu
from jax.sharding import PartitionSpec as P


HD = 128
AXES = ("seq", "section", "head")
F32 = jnp.float32
BF16 = jnp.bfloat16
VMEM = pl.BlockSpec(memory_space=pltpu.VMEM)
HBM = pl.BlockSpec(memory_space=pltpu.HBM)
SMEM = pl.BlockSpec(memory_space=pltpu.SMEM)
MIB = 1 << 20


def permute(value, sizes, target):
    pairs = []
    for s in range(sizes[0]):
        for c in range(sizes[1]):
            for h in range(sizes[2]):
                ts, tc, th = target(s, c, h)
                at = (s * sizes[1] + c) * sizes[2] + h
                to = (ts * sizes[1] + tc) * sizes[2] + th
                pairs.append((at, to))
    return lax.ppermute(value, AXES, pairs)


def rms(values, gain):
    mean_sq = jnp.mean(values * values, axis=-1, keepdims=True)
    return values * lax.rsqrt(mean_sq + 1e-06) * gain


def dot(a, b, dims=((1,), (0,))):
    return lax.dot_general(a, b, (dims, ((), ())), preferred_element_type=F32)


def tree_sum(terms):
    terms = [t.astype(F32) for t in terms]
    while len(terms) > 1:
        terms = [sum(terms[i : i + 2]) for i in range(0, len(terms), 2)]
    return terms[0]


def masked(values, first, length):
    at = first + lax.broadcasted_iota(jnp.int32, values.shape, 0)
    return jnp.where(at < length, values, 0.0)


def first_latent_body(spans, rows, *refs):
    x_hbm, gain_hbm, w_hbm, lgain_hbm, normed_ref, full_ref = refs[:6]
    latent_refs = refs[6 : 6 + len(spans)]
    x_ref, gain_ref, lgain_ref, w_ref, sems = refs[6 + len(spans) :]
    copies = [
        pltpu.make_async_copy(source, to, sems.at[i])
        for i, (source, to) in enumerate(
            ((x_hbm, x_ref), (gain_hbm, gain_ref), (lgain_hbm, lgain_ref), (w_hbm, w_ref))
        )
    ]
    for copy in copies:
        copy.start()
    copies[0].wait()
    copies[1].wait()
    normed = rms(x_ref[...].astype(F32), gain_ref[...]).astype(BF16)
    normed_ref[...] = normed
    copies[2].wait()
    copies[3].wait()
    full = rms(dot(normed, w_ref[...]), lgain_ref[...])
    full_ref[...] = full
    latent = full.astype(BF16)
    for (low, high), latent_ref in zip(spans, latent_refs):
        latent_ref[...] = latent[low * rows : high * rows]


def next_latent_body(span, rows, n_parts, where_ref, lengths_ref, *refs):
    x_ref = refs[0]
    parts = refs[1 : 1 + n_parts]
    refs = refs[1 + n_parts :]
    gain_ref, w_ref, lgain_ref, before_ref, state_ref, normed_ref, live_ref, latent_ref = refs
    low, high = span
    span_rows = slice(low * rows, high * rows)
    state = x_ref[span_rows].astype(F32) + tree_sum([p[...] for p in parts])
    state_ref[...] = state
    normed = rms(state, gain_ref[...]).astype(BF16)
    normed_ref[...] = normed
    full = rms(dot(normed, w_ref[...]), lgain_ref[...])
    latent_ref[...] = full.astype(BF16)
    second = jnp.broadcast_to(where_ref[1], (rows, full.shape[1])) == 1
    for g in range(low, high):
        at = slice((g - low) * rows, (g - low + 1) * rows)
        mine = jnp.where(second, full[at], before_ref[g * rows : (g + 1) * rows])
        live_ref[at] = masked(mine, where_ref[0] * rows, lengths_ref[g])


def query_body(scale, normed_ref, wq_ref, wk_ref, out_ref):
    heads = out_ref.shape[0]
    query = dot(normed_ref[...], wq_ref[...]).astype(BF16)
    for h in range(heads):
        cols = slice(h * HD, (h + 1) * HD)
        one = dot(query[:, cols], wk_ref[:, cols], ((1,), (1,)))
        out_ref[h] = (one * scale).astype(BF16)


def attention(spans, rows, n_pieces, offset, where_ref, lengths_ref, absorbed_ref, pieces, wv, kv, attn):
    heads = absorbed_ref.shape[0]
    rank = kv.shape[1]
    block = n_pieces * rows
    me = where_ref[0]
    for i, (low, high) in enumerate(spans):
        for g in range(low, high):
            for k in range(n_pieces):
                piece = pieces[i * n_pieces + k]
                kv[pl.ds(g * block + k * rows, rows), :] = piece[pl.ds((g - low) * rows, rows), :]
    col = lax.broadcasted_iota(jnp.int32, (rows, block), 1)
    row = lax.broadcasted_iota(jnp.int32, (rows, block), 0)
    key_pos = jnp.bitwise_xor(me, col // rows) * rows + col % rows
    query_pos = me * rows + row
    causal = key_pos <= query_pos
    low, high = spans[-1]
    for g in range(low, high):
        keys = kv[: (g + 1) * block, :]
        at = g * rows - offset
        absorbed = absorbed_ref[:, at : at + rows, :].reshape(heads * rows, rank)
        scores = dot(absorbed, keys, ((1,), (1,)))
        mask = [key_pos < lengths_ref[b] for b in range(g)] + [causal]
        mask = jnp.concatenate(mask, axis=1)[None]
        scores = scores.reshape(heads, rows, (g + 1) * block)
        scores = jnp.where(mask, scores, -1e30)
        top = jnp.max(scores, axis=2, keepdims=True)
        weights = jnp.where(mask, jnp.exp(scores - top), 0.0)
        total = jnp.sum(weights, axis=2, keepdims=True).reshape(heads * rows, 1)
        rounded = weights.astype(BF16).reshape(heads * rows, (g + 1) * block)
        context = (dot(rounded, keys) / total).astype(BF16)
        at = (g - low) * rows
        for h in range(heads):
            cols = slice(h * HD, (h + 1) * HD)
            one = dot(context[h * rows : (h + 1) * rows], wv[:, cols])
            attn[at : at + rows, cols] = one.astype(BF16)


def attend_body(spans, rows, n_pieces, offset, where_ref, lengths_ref, absorbed_ref, *refs):
    n_in = len(spans) * n_pieces
    pieces = refs[:n_in]
    wv, wo, out_ref, kv, attn = refs[n_in:]
    attention(
        spans, rows, n_pieces, offset, where_ref, lengths_ref, absorbed_ref, pieces, wv, kv, attn
    )
    out_ref[...] = dot(attn[...], wo[...]).astype(BF16)


def attend_last_body(
    spans, rows, n_pieces, offset, n_head, n_sec, where_ref, lengths_ref, absorbed_ref, *refs
):
    n_in = len(spans) * n_pieces
    pieces = refs[:n_in]
    wv, wo, state_ref, keep_ref, give_ref = refs[n_in : n_in + 5]
    sends = refs[n_in + 5 : n_in + 4 + n_head]
    kv, attn, total = refs[n_in + 4 + n_head :]
    attention(
        spans, rows, n_pieces, offset, where_ref, lengths_ref, absorbed_ref, pieces, wv, kv, attn
    )
    total[...] = dot(attn[...], wo[...])
    low, high = spans[-1]
    share = rows // n_head
    width = total.shape[1]
    part = width // n_sec
    for g in range(high - low):
        to = slice(g * share, (g + 1) * share)

        def at(h):
            return pl.ds(pl.multiple_of(g * rows + h * share, share), share)

        own = at(where_ref[2])
        mine = state_ref[own, :] + total[own, :]
        give_ref[to] = mine[:, : width - part].astype(BF16)
        keep_ref[to] = mine[:, width - part :]
        for k in range(1, n_head):
            sends[k - 1][to] = total[at(jnp.bitwise_xor(where_ref[2], k)), :].astype(BF16)


def final_body(spans, rows, n_head, n_sec, where_ref, lengths_ref, *refs):
    out_ref = refs[-1]
    per = 2 + 2 * (n_head - 1)
    share = rows // n_head
    part = out_ref.shape[2]
    first = where_ref[0] * rows + where_ref[2] * share
    for i, (low, high) in enumerate(spans):
        keep, given = refs[i * per : i * per + 2]
        came = refs[i * per + 2 : i * per + 1 + n_head]
        relay = refs[i * per + 1 + n_head : (i + 1) * per]
        last = jnp.broadcast_to(where_ref[1], (share, part)) == n_sec - 1
        for g in range(low, high):
            at = slice((g - low) * share, (g - low + 1) * share)
            here = keep[at]
            there = given[at].astype(F32)
            for k in range(n_head - 1):
                here = here + relay[k][at, (n_sec - 1) * part :].astype(F32)
                there = there + came[k][at, :part].astype(F32)
            out_ref[g] = masked(jnp.where(last, here, there), first, lengths_ref[g])


def in_hbm(value):
    return pltpu.with_memory_space_constraint(value, pltpu.HBM)


def params(limit):
    return pltpu.CompilerParams(vmem_limit_bytes=limit * MIB)


def array(dtype, *shape):
    return jax.ShapeDtypeStruct(shape, dtype)


def cost(flops, moved, exps=0):
    return pl.CostEstimate(flops=flops, bytes_accessed=moved, transcendentals=exps)


def after(value, *others):
    return lax.optimization_barrier((value, *others))[0]


def shards(hidden, lengths, attn_gain, w_query, w_latent, latent_gain, w_key, w_value, w_out):
    n_seq = lax.axis_size("seq")
    n_sec = lax.axis_size("section")
    n_head = lax.axis_size("head")
    assert n_sec == 2
    sizes = (n_seq, n_sec, n_head)
    where = jnp.stack([lax.axis_index(axis) for axis in AXES]).astype(jnp.int32)
    groups, rows, width = hidden.shape
    rank = w_latent.shape[2]
    heads = w_key.shape[2] // HD
    total_rows = groups * rows
    share = rows // n_head
    part_width = width // n_sec
    x = hidden.reshape(total_rows, width)
    wl, wq, wk, wv, wo = w_latent[0], w_query[0], w_key[0], w_value[0], w_out[0]
    cut = max(1, groups - 1)
    spans = [(0, cut), (cut, groups)] if cut < groups else [(0, groups)]
    span_size = [(high - low) * rows for low, high in spans]

    def first_latent():
        out = pl.pallas_call(
            functools.partial(first_latent_body, spans, rows),
            out_shape=(
                array(BF16, total_rows, width),
                array(F32, total_rows, rank),
                *(array(BF16, size, rank) for size in span_size),
            ),
            in_specs=[HBM] * 4,
            out_specs=(VMEM,) * (2 + len(spans)),
            scratch_shapes=[
                pltpu.VMEM((total_rows, width), BF16),
                pltpu.VMEM((1, width), F32),
                pltpu.VMEM((1, rank), F32),
                pltpu.VMEM((width, rank), BF16),
                pltpu.SemaphoreType.DMA((4,)),
            ],
            compiler_params=params(12),
            name="first_latent",
        )(*(in_hbm(value) for value in (x, attn_gain, wl, latent_gain)))
        return out[0], out[1], list(out[2:])

    def next_latent(i, parts, before):
        size = span_size[i]
        return pl.pallas_call(
            functools.partial(next_latent_body, spans[i], rows, len(parts)),
            out_shape=(
                array(F32, size, width),
                array(BF16, size, width),
                array(F32, size, rank),
                array(BF16, size, rank),
            ),
            in_specs=[SMEM] * 2 + [VMEM] * (5 + len(parts)),
            out_specs=(VMEM,) * 4,
            compiler_params=params(8),
            cost_estimate=cost(2 * size * width * rank, 2 * width * (rank + 2 * size)),
        )(where, lengths, x, *parts, attn_gain, wl, latent_gain, before)

    def project(normed):
        size = normed.shape[0]
        return pl.pallas_call(
            functools.partial(query_body, 1.0 / HD**0.5),
            out_shape=array(BF16, heads, size, rank),
            in_specs=[VMEM] * 3,
            out_specs=VMEM,
            compiler_params=params(8),
            cost_estimate=cost(
                2 * size * heads * HD * (width + rank), 2 * heads * HD * (width + rank + size)
            ),
        )(normed, wq, wk)

    def attend(i, absorbed, offset, pieces, state=None):
        which = spans[: i + 1]
        high = spans[i][1]
        size = span_size[i]
        flat = [piece for of_span in pieces[: i + 1] for piece in of_span]
        scratch = [
            pltpu.VMEM((high * n_seq * rows, rank), BF16),
            pltpu.VMEM((size, heads * HD), BF16),
        ]
        common = dict(
            compiler_params=params(20),
            cost_estimate=cost(
                4 * heads * size * high * n_seq * rows * rank,
                2 * heads * HD * (width + rank),
                heads * size * high * n_seq * rows,
            ),
        )
        if state is None:
            return pl.pallas_call(
                functools.partial(attend_body, which, rows, n_seq, offset),
                out_shape=array(BF16, size, width),
                in_specs=[SMEM, SMEM] + [VMEM] * (3 + len(flat)),
                out_specs=VMEM,
                scratch_shapes=scratch,
                **common,
            )(where, lengths, absorbed, *flat, wv, wo)
        small = size // n_head
        return pl.pallas_call(
            functools.partial(attend_last_body, which, rows, n_seq, offset, n_head, n_sec),
            out_shape=(
                array(F32, small, part_width),
                array(BF16, small, width - part_width),
                *(array(BF16, small, width) for _ in range(n_head - 1)),
            ),
            in_specs=[SMEM, SMEM] + [VMEM] * (4 + len(flat)),
            out_specs=(VMEM,) * (1 + n_head),
            scratch_shapes=scratch + [pltpu.VMEM((size, width), F32)],
            **common,
        )(where, lengths, absorbed, *flat, wv, wo, state)

    def swap(value):
        return permute(value, sizes, lambda s, c, h: (s, 1 - c, h))

    def cross(value, source, k):
        return permute(
            value, sizes, lambda s, c, h: (s, 1 - c, h ^ k) if c == source else (s, 1 - c, h)
        )

    def gather(latent, tick):
        there = swap(latent)
        return [latent] + [
            permute(
                there, sizes, lambda s, c, h, k=k: (s, 1 - c, h) if c == tick else (s ^ k, tick, h)
            )
            for k in range(1, n_seq)
        ]

    def hand_on(partial):
        return [swap(partial)] + [cross(partial, 0, k) for k in range(1, n_head)]

    normed, full, latents = first_latent()
    pieces = [gather(latent, 0) for latent in latents]
    absorbed = project(normed)
    parts = [hand_on(attend(i, absorbed, 0, pieces)) for i in range(len(spans))]
    pieces, queries, states, lives = [], [], [], []
    for i in range(len(spans)):
        part = parts[i]
        if i:
            part = [after(p, queries[-1]) for p in part]
        state, normed, stored, latent = next_latent(i, part, full)
        states.append(state)
        lives.append(stored)
        pieces.append(gather(latent, 1))
        queries.append(project(normed))
    ends = []
    for i in range(len(spans)):
        keep, give, *sends = attend(i, queries[i], spans[i][0] * rows, pieces, states[i])
        given = swap(give)
        came = [cross(sends[k - 1], 1, k) for k in range(1, n_head)]
        relay = [swap(one) for one in came]
        ends += [keep, given, *came, *relay]
    final = pl.pallas_call(
        functools.partial(final_body, spans, rows, n_head, n_sec),
        out_shape=array(F32, groups, share, part_width),
        in_specs=[SMEM] * 2 + [VMEM] * len(ends),
        out_specs=VMEM,
        compiler_params=params(12),
        name="final",
    )(where, lengths, *ends)
    stored = jnp.concatenate(lives, 0).reshape(1, groups, rows, rank)
    return (final, stored)


def solution(mesh):
    return jax.shard_map(
        shards,
        mesh=mesh,
        in_specs=(
            P("rep", "seq", None),
            P("rep"),
            P("section", None),
            P("section", None, "head"),
            P("section", None, None),
            P("section", None),
            P("section", None, "head"),
            P("section", None, "head"),
            P("section", "head", None),
        ),
        out_specs=(P("rep", ("seq", "head"), "section"), P("section", "rep", "seq", None)),
        check_vma=False,
    )
```

```python
import functools

import jax
import jax.numpy as jnp
from jax import lax
from jax.experimental import pallas as pl
from jax.experimental.pallas import tpu as pltpu
from jax.sharding import PartitionSpec as P


HD = 128
AXES = ("seq", "section", "head")
F32 = jnp.float32
BF16 = jnp.bfloat16
VMEM = pl.BlockSpec(memory_space=pltpu.VMEM)
HBM = pl.BlockSpec(memory_space=pltpu.HBM)
SMEM = pl.BlockSpec(memory_space=pltpu.SMEM)
MIB = 1 << 20


def permute(value, sizes, target):
    pairs = []
    for s in range(sizes[0]):
        for c in range(sizes[1]):
            for h in range(sizes[2]):
                ts, tc, th = target(s, c, h)
                at = (s * sizes[1] + c) * sizes[2] + h
                to = (ts * sizes[1] + tc) * sizes[2] + th
                pairs.append((at, to))
    return lax.ppermute(value, AXES, pairs)


def rms(values, gain):
    mean_sq = jnp.mean(values * values, axis=-1, keepdims=True)
    return values * lax.rsqrt(mean_sq + 1e-06) * gain


def dot(a, b, dims=((1,), (0,))):
    return lax.dot_general(a, b, (dims, ((), ())), preferred_element_type=F32)


def tree_sum(terms):
    terms = [t.astype(F32) for t in terms]
    while len(terms) > 1:
        terms = [sum(terms[i : i + 2]) for i in range(0, len(terms), 2)]
    return terms[0]


def place(axis):
    return lax.axis_index(axis).astype(jnp.int32)


def alive(at, length):
    return jnp.where(at < length, 1.0, 0.0)


def prepare_body(rows, n_pieces, lengths_ref, bias_ref, live_ref, final_ref):
    groups = lengths_ref.shape[0]
    block = n_pieces * rows
    me = place("seq")
    col = lax.broadcasted_iota(jnp.int32, (rows, block), 1)
    row = lax.broadcasted_iota(jnp.int32, (rows, block), 0)
    key_pos = jnp.bitwise_xor(me, col // rows) * rows + col % rows
    for g in range(groups):
        bias_ref[:, g * block : (g + 1) * block] = jnp.where(key_pos < lengths_ref[g], 0.0, -1e30)
    bias_ref[:, groups * block :] = jnp.where(key_pos <= me * rows + row, 0.0, -1e30)
    share = final_ref.shape[0] // groups
    lanes = live_ref.shape[1]
    at = me * rows + lax.broadcasted_iota(jnp.int32, (rows, lanes), 0)
    shared_at = me * rows + place("head") * share
    shared_at = shared_at + lax.broadcasted_iota(jnp.int32, (share, lanes), 0)
    for g in range(groups):
        live_ref[g * rows : (g + 1) * rows] = alive(at, lengths_ref[g])
        final_ref[g * share : (g + 1) * share] = alive(shared_at, lengths_ref[g])


def keep_live(values, live):
    return jnp.where(live[:, :1] > 0.5, values, 0.0)


def first_latent_body(spans, rows, cuts, *refs):
    x_hbm, gain_hbm, w_hbm, lgain_hbm, normed_ref, full_ref = refs[:6]
    latent_refs = refs[6 : 6 + len(spans)]
    x_ref, gain_ref, lgain_ref, w_ref, sems = refs[6 + len(spans) :]
    copies = [
        pltpu.make_async_copy(source, to, sems.at[i])
        for i, (source, to) in enumerate(
            ((x_hbm, x_ref), (gain_hbm, gain_ref), (lgain_hbm, lgain_ref))
        )
    ]
    depth = w_ref.shape[0] // cuts
    tiles = [slice(i * depth, (i + 1) * depth) for i in range(cuts)]
    for i, tile in enumerate(tiles):
        copies.append(pltpu.make_async_copy(w_hbm.at[tile], w_ref.at[tile], sems.at[3 + i]))
    for copy in copies:
        copy.start()
    copies[0].wait()
    copies[1].wait()
    normed = rms(x_ref[...].astype(F32), gain_ref[...]).astype(BF16)
    normed_ref[...] = normed
    copies[2].wait()
    raw = None
    for i, tile in enumerate(tiles):
        copies[3 + i].wait()
        one = dot(normed[:, tile], w_ref[tile])
        raw = one if raw is None else raw + one
    full = rms(raw, lgain_ref[...])
    full_ref[...] = full
    latent = full.astype(BF16)
    for (low, high), latent_ref in zip(spans, latent_refs):
        latent_ref[...] = latent[low * rows : high * rows]


def next_latent_body(span, rows, n_parts, *refs):
    x_ref = refs[0]
    parts = refs[1 : 1 + n_parts]
    refs = refs[1 + n_parts :]
    gain_ref, w_ref, lgain_ref, before_ref, live_ref = refs[:5]
    state_ref, normed_ref, stored_ref, latent_ref = refs[5:]
    at = slice(span[0] * rows, span[1] * rows)
    state = x_ref[at].astype(F32) + tree_sum([p[...] for p in parts])
    state_ref[...] = state
    normed = rms(state, gain_ref[...]).astype(BF16)
    normed_ref[...] = normed
    full = rms(dot(normed, w_ref[...]), lgain_ref[...])
    latent_ref[...] = full.astype(BF16)
    second = jnp.broadcast_to(place("section"), full.shape) == 1
    stored_ref[...] = keep_live(jnp.where(second, full, before_ref[at]), live_ref[at])


def absorb(scale, query, wk, out_ref):
    for h in range(out_ref.shape[0]):
        cols = slice(h * HD, (h + 1) * HD)
        one = dot(query[:, cols], wk[:, cols], ((1,), (1,)))
        out_ref[h] = (one * scale).astype(BF16)


def first_query_body(scale, cuts, normed_ref, wq_hbm, wk_hbm, out_ref, wq, wk, sems):
    depth = wq.shape[0] // cuts
    tiles = [slice(i * depth, (i + 1) * depth) for i in range(cuts)]
    copies = [
        pltpu.make_async_copy(wq_hbm.at[tile], wq.at[tile], sems.at[i])
        for i, tile in enumerate(tiles)
    ]
    copies.append(pltpu.make_async_copy(wk_hbm, wk, sems.at[cuts]))
    for copy in copies:
        copy.start()
    query = None
    for i, tile in enumerate(tiles):
        copies[i].wait()
        one = dot(normed_ref[:, tile], wq[tile])
        query = one if query is None else query + one
    copies[cuts].wait()
    absorb(scale, query.astype(BF16), wk, out_ref)


def query_body(scale, normed_ref, wq_ref, wk_ref, out_ref):
    absorb(scale, dot(normed_ref[...], wq_ref[...]).astype(BF16), wk_ref, out_ref)


def attention(spans, rows, n_pieces, offset, absorbed_ref, bias_ref, pieces, wv, kv, ctx, attn):
    heads = absorbed_ref.shape[0]
    rank = kv.shape[1]
    block = n_pieces * rows
    for i, (low, high) in enumerate(spans):
        for g in range(low, high):
            for k in range(n_pieces):
                piece = pieces[i * n_pieces + k]
                kv[pl.ds(g * block + k * rows, rows), :] = piece[pl.ds((g - low) * rows, rows), :]
    low, high = spans[-1]
    causal = bias_ref[:, bias_ref.shape[1] - block :]
    for g in range(low, high):
        keys = kv[: (g + 1) * block, :]
        at = g * rows - offset
        absorbed = absorbed_ref[:, at : at + rows, :].reshape(heads * rows, rank)
        scores = dot(absorbed, keys, ((1,), (1,))).reshape(heads, rows, (g + 1) * block)
        bias = jnp.concatenate([bias_ref[:, : g * block], causal], axis=1) if g else causal
        scores = scores + bias[None]
        weights = jnp.exp(scores - jnp.max(scores, axis=2, keepdims=True))
        total = jnp.sum(weights, axis=2, keepdims=True).reshape(heads * rows, 1)
        rounded = weights.astype(BF16).reshape(heads * rows, (g + 1) * block)
        context = (dot(rounded, keys) * (1.0 / total)).astype(BF16)
        at = (g - low) * rows
        ctx[:, at : at + rows, :] = context.reshape(heads, rows, rank)
    for h in range(heads):
        cols = slice(h * HD, (h + 1) * HD)
        attn[:, cols] = dot(ctx[h], wv[:, cols]).astype(BF16)


def attend_body(spans, rows, n_pieces, offset, absorbed_ref, bias_ref, *refs):
    n_in = len(spans) * n_pieces
    pieces = refs[:n_in]
    wv, wo, out_ref, kv, ctx, attn = refs[n_in:]
    attention(spans, rows, n_pieces, offset, absorbed_ref, bias_ref, pieces, wv, kv, ctx, attn)
    out_ref[...] = dot(attn[...], wo[...]).astype(BF16)


def attend_last_body(spans, rows, n_pieces, offset, n_head, n_sec, absorbed_ref, bias_ref, *refs):
    n_in = len(spans) * n_pieces
    pieces = refs[:n_in]
    wv, wo, state_ref, keep_ref, give_ref = refs[n_in : n_in + 5]
    sends = refs[n_in + 5 : n_in + 4 + n_head]
    kv, ctx, attn, total = refs[n_in + 4 + n_head :]
    attention(spans, rows, n_pieces, offset, absorbed_ref, bias_ref, pieces, wv, kv, ctx, attn)
    total[...] = dot(attn[...], wo[...])
    low, high = spans[-1]
    share = rows // n_head
    width = total.shape[1]
    part = width // n_sec
    head = place("head")
    for g in range(high - low):
        to = slice(g * share, (g + 1) * share)

        def at(h):
            return pl.ds(pl.multiple_of(g * rows + h * share, share), share)

        mine = state_ref[at(head), :] + total[at(head), :]
        give_ref[to] = mine[:, : width - part].astype(BF16)
        keep_ref[to] = mine[:, width - part :]
        for k in range(1, n_head):
            sends[k - 1][to] = total[at(jnp.bitwise_xor(head, k)), :].astype(BF16)


def final_body(spans, rows, n_head, n_sec, final_ref, *refs):
    out_ref = refs[-1]
    per = 2 + 2 * (n_head - 1)
    share = rows // n_head
    part = out_ref.shape[2]
    last = jnp.broadcast_to(place("section"), (share, part)) == n_sec - 1
    for i, (low, high) in enumerate(spans):
        keep, given = refs[i * per : i * per + 2]
        came = refs[i * per + 2 : i * per + 1 + n_head]
        relay = refs[i * per + 1 + n_head : (i + 1) * per]
        for g in range(low, high):
            at = slice((g - low) * share, (g - low + 1) * share)
            here = keep[at]
            there = given[at].astype(F32)
            for k in range(n_head - 1):
                here = here + relay[k][at, (n_sec - 1) * part :].astype(F32)
                there = there + came[k][at, :part].astype(F32)
            live = final_ref[g * share : (g + 1) * share]
            out_ref[g] = keep_live(jnp.where(last, here, there), live)


def in_hbm(value):
    return pltpu.with_memory_space_constraint(value, pltpu.HBM)


def params(limit):
    return pltpu.CompilerParams(vmem_limit_bytes=limit * MIB)


def array(dtype, *shape):
    return jax.ShapeDtypeStruct(shape, dtype)


def cost(flops, moved, exps=0):
    return pl.CostEstimate(flops=flops, bytes_accessed=moved, transcendentals=exps)


def after(value, *others):
    return lax.optimization_barrier((value, *others))[0]


def shards(hidden, lengths, attn_gain, w_query, w_latent, latent_gain, w_key, w_value, w_out):
    n_seq = lax.axis_size("seq")
    n_sec = lax.axis_size("section")
    n_head = lax.axis_size("head")
    assert n_sec == 2
    sizes = (n_seq, n_sec, n_head)
    groups, rows, width = hidden.shape
    rank = w_latent.shape[2]
    heads = w_key.shape[2] // HD
    total_rows = groups * rows
    share = rows // n_head
    part_width = width // n_sec
    x = hidden.reshape(total_rows, width)
    wl, wq, wk, wv, wo = w_latent[0], w_query[0], w_key[0], w_value[0], w_out[0]
    cut = max(1, groups - 1)
    cuts = 4
    spans = [(0, cut), (cut, groups)] if cut < groups else [(0, groups)]
    span_size = [(high - low) * rows for low, high in spans]

    def prepare():
        return pl.pallas_call(
            functools.partial(prepare_body, rows, n_seq),
            out_shape=(
                array(F32, rows, (groups + 1) * n_seq * rows),
                array(F32, total_rows, HD),
                array(F32, groups * share, HD),
            ),
            in_specs=[SMEM],
            out_specs=(VMEM,) * 3,
            compiler_params=params(8),
            name="prepare",
        )(lengths)

    def first_latent():
        out = pl.pallas_call(
            functools.partial(first_latent_body, spans, rows, cuts),
            out_shape=(
                array(BF16, total_rows, width),
                array(F32, total_rows, rank),
                *(array(BF16, size, rank) for size in span_size),
            ),
            in_specs=[HBM] * 4,
            out_specs=(VMEM,) * (2 + len(spans)),
            scratch_shapes=[
                pltpu.VMEM((total_rows, width), BF16),
                pltpu.VMEM((1, width), F32),
                pltpu.VMEM((1, rank), F32),
                pltpu.VMEM((width, rank), BF16),
                pltpu.SemaphoreType.DMA((3 + cuts,)),
            ],
            compiler_params=params(12),
            name="first_latent",
        )(*(in_hbm(value) for value in (x, attn_gain, wl, latent_gain)))
        return out[0], out[1], list(out[2:])

    def next_latent(i, parts, before):
        size = span_size[i]
        return pl.pallas_call(
            functools.partial(next_latent_body, spans[i], rows, len(parts)),
            out_shape=(
                array(F32, size, width),
                array(BF16, size, width),
                array(F32, size, rank),
                array(BF16, size, rank),
            ),
            in_specs=[VMEM] * (6 + len(parts)),
            out_specs=(VMEM,) * 4,
            compiler_params=params(8),
            cost_estimate=cost(2 * size * width * rank, 2 * width * (rank + 2 * size)),
        )(x, *parts, attn_gain, wl, latent_gain, before, live)

    def project(normed):
        size = normed.shape[0]
        return pl.pallas_call(
            functools.partial(query_body, 1.0 / HD**0.5),
            out_shape=array(BF16, heads, size, rank),
            in_specs=[VMEM] * 3,
            out_specs=VMEM,
            compiler_params=params(8),
            cost_estimate=cost(
                2 * size * heads * HD * (width + rank), 2 * heads * HD * (width + rank + size)
            ),
        )(normed, wq, wk)

    def first_project(normed):
        size = normed.shape[0]
        return pl.pallas_call(
            functools.partial(first_query_body, 1.0 / HD**0.5, cuts),
            out_shape=array(BF16, heads, size, rank),
            in_specs=[VMEM, HBM, HBM],
            out_specs=VMEM,
            scratch_shapes=[
                pltpu.VMEM((width, heads * HD), BF16),
                pltpu.VMEM((rank, heads * HD), BF16),
                pltpu.SemaphoreType.DMA((cuts + 1,)),
            ],
            compiler_params=params(14),
            cost_estimate=cost(
                2 * size * heads * HD * (width + rank), 2 * heads * HD * (width + rank + size)
            ),
        )(normed, in_hbm(wq), in_hbm(wk))

    def attend(i, absorbed, offset, pieces, state=None):
        which = spans[: i + 1]
        high = spans[i][1]
        size = span_size[i]
        flat = [piece for of_span in pieces[: i + 1] for piece in of_span]
        scratch = [
            pltpu.VMEM((high * n_seq * rows, rank), BF16),
            pltpu.VMEM((heads, size, rank), BF16),
            pltpu.VMEM((size, heads * HD), BF16),
        ]
        common = dict(
            compiler_params=params(20),
            cost_estimate=cost(
                4 * heads * size * high * n_seq * rows * rank,
                2 * heads * HD * (width + rank),
                heads * size * high * n_seq * rows,
            ),
        )
        if state is None:
            return pl.pallas_call(
                functools.partial(attend_body, which, rows, n_seq, offset),
                out_shape=array(BF16, size, width),
                in_specs=[VMEM] * (4 + len(flat)),
                out_specs=VMEM,
                scratch_shapes=scratch,
                **common,
            )(absorbed, bias, *flat, wv, wo)
        small = size // n_head
        return pl.pallas_call(
            functools.partial(attend_last_body, which, rows, n_seq, offset, n_head, n_sec),
            out_shape=(
                array(F32, small, part_width),
                array(BF16, small, width - part_width),
                *(array(BF16, small, width) for _ in range(n_head - 1)),
            ),
            in_specs=[VMEM] * (5 + len(flat)),
            out_specs=(VMEM,) * (1 + n_head),
            scratch_shapes=scratch + [pltpu.VMEM((size, width), F32)],
            **common,
        )(absorbed, bias, *flat, wv, wo, state)

    def swap(value):
        return permute(value, sizes, lambda s, c, h: (s, 1 - c, h))

    def cross(value, source, k):
        return permute(
            value, sizes, lambda s, c, h: (s, 1 - c, h ^ k) if c == source else (s, 1 - c, h)
        )

    def gather(latent, tick):
        there = swap(latent)
        return [latent] + [
            permute(
                there, sizes, lambda s, c, h, k=k: (s, 1 - c, h) if c == tick else (s ^ k, tick, h)
            )
            for k in range(1, n_seq)
        ]

    def hand_on(partial):
        return [swap(partial)] + [cross(partial, 0, k) for k in range(1, n_head)]

    normed, full, latents = first_latent()
    pieces = [gather(latent, 0) for latent in latents]
    bias, live, final_live = prepare()
    absorbed = first_project(normed)
    parts = [hand_on(attend(i, absorbed, 0, pieces)) for i in range(len(spans))]
    pieces, queries, states, lives = [], [], [], []
    for i in range(len(spans)):
        part = parts[i]
        if i:
            part = [after(p, queries[-1]) for p in part]
        state, normed, stored, latent = next_latent(i, part, full)
        states.append(state)
        lives.append(stored)
        pieces.append(gather(latent, 1))
        queries.append(project(normed))
    ends = []
    for i in range(len(spans)):
        keep, give, *sends = attend(i, queries[i], spans[i][0] * rows, pieces, states[i])
        given = swap(give)
        came = [cross(sends[k - 1], 1, k) for k in range(1, n_head)]
        relay = [swap(one) for one in came]
        ends += [keep, given, *came, *relay]
    final = pl.pallas_call(
        functools.partial(final_body, spans, rows, n_head, n_sec),
        out_shape=array(F32, groups, share, part_width),
        in_specs=[VMEM] * (1 + len(ends)),
        out_specs=VMEM,
        compiler_params=params(12),
        name="final",
    )(final_live, *ends)
    stored = jnp.concatenate(lives, 0).reshape(1, groups, rows, rank)
    return (final, stored)


def solution(mesh):
    return jax.shard_map(
        shards,
        mesh=mesh,
        in_specs=(
            P("rep", "seq", None),
            P("rep"),
            P("section", None),
            P("section", None, "head"),
            P("section", None, None),
            P("section", None),
            P("section", None, "head"),
            P("section", None, "head"),
            P("section", "head", None),
        ),
        out_specs=(P("rep", ("seq", "head"), "section"), P("section", "rep", "seq", None)),
        check_vma=False,
    )
```

```python
import functools

import jax
import jax.numpy as jnp
from jax import lax
from jax.experimental import pallas as pl
from jax.experimental.pallas import tpu as pltpu
from jax.sharding import PartitionSpec as P


HD = 128
AXES = ("seq", "section", "head")
F32 = jnp.float32
BF16 = jnp.bfloat16
VMEM = pl.BlockSpec(memory_space=pltpu.VMEM)
HBM = pl.BlockSpec(memory_space=pltpu.HBM)
SMEM = pl.BlockSpec(memory_space=pltpu.SMEM)
MIB = 1 << 20


def permute(value, sizes, target):
    pairs = []
    for s in range(sizes[0]):
        for c in range(sizes[1]):
            for h in range(sizes[2]):
                ts, tc, th = target(s, c, h)
                at = (s * sizes[1] + c) * sizes[2] + h
                to = (ts * sizes[1] + tc) * sizes[2] + th
                pairs.append((at, to))
    return lax.ppermute(value, AXES, pairs)


def rms(values, gain):
    mean_sq = jnp.mean(values * values, axis=-1, keepdims=True)
    return values * lax.rsqrt(mean_sq + 1e-06) * gain


def dot(a, b, dims=((1,), (0,))):
    return lax.dot_general(a, b, (dims, ((), ())), preferred_element_type=F32)


def tree_sum(terms):
    terms = [t.astype(F32) for t in terms]
    while len(terms) > 1:
        terms = [sum(terms[i : i + 2]) for i in range(0, len(terms), 2)]
    return terms[0]


def place(axis):
    return lax.axis_index(axis).astype(jnp.int32)


def in_turn(section, work, *outs):
    pl.when(place("section") == section)(work)

    @pl.when(place("section") != section)
    def _():
        for out in outs:
            out[...] = jnp.zeros_like(out)


def alive(at, length):
    return jnp.where(at < length, 1.0, 0.0)


def prepare_body(rows, n_pieces, lengths_ref, bias_ref, live_ref, final_ref):
    groups = lengths_ref.shape[0]
    block = n_pieces * rows
    me = place("seq")
    col = lax.broadcasted_iota(jnp.int32, (rows, block), 1)
    row = lax.broadcasted_iota(jnp.int32, (rows, block), 0)
    key_pos = jnp.bitwise_xor(me, col // rows) * rows + col % rows
    for g in range(groups):
        bias_ref[:, g * block : (g + 1) * block] = jnp.where(key_pos < lengths_ref[g], 0.0, -1e30)
    bias_ref[:, groups * block :] = jnp.where(key_pos <= me * rows + row, 0.0, -1e30)
    share = final_ref.shape[0] // groups
    lanes = live_ref.shape[1]
    at = me * rows + lax.broadcasted_iota(jnp.int32, (rows, lanes), 0)
    shared_at = me * rows + place("head") * share
    shared_at = shared_at + lax.broadcasted_iota(jnp.int32, (share, lanes), 0)
    for g in range(groups):
        live_ref[g * rows : (g + 1) * rows] = alive(at, lengths_ref[g])
        final_ref[g * share : (g + 1) * share] = alive(shared_at, lengths_ref[g])


def keep_live(values, live):
    return jnp.where(live[:, :1] > 0.5, values, 0.0)


def first_latent_body(spans, rows, cuts, *refs):
    x_hbm, gain_hbm, w_hbm, lgain_hbm, normed_ref, full_ref = refs[:6]
    latent_refs = refs[6 : 6 + len(spans)]
    x_ref, gain_ref, lgain_ref, w_ref, sems = refs[6 + len(spans) :]

    def work():
        copies = [
            pltpu.make_async_copy(source, to, sems.at[i])
            for i, (source, to) in enumerate(
                ((x_hbm, x_ref), (gain_hbm, gain_ref), (lgain_hbm, lgain_ref))
            )
        ]
        depth = w_ref.shape[0] // cuts
        tiles = [slice(i * depth, (i + 1) * depth) for i in range(cuts)]
        for i, tile in enumerate(tiles):
            copies.append(pltpu.make_async_copy(w_hbm.at[tile], w_ref.at[tile], sems.at[3 + i]))
        for copy in copies:
            copy.start()
        copies[0].wait()
        copies[1].wait()
        normed = rms(x_ref[...].astype(F32), gain_ref[...]).astype(BF16)
        normed_ref[...] = normed
        copies[2].wait()
        raw = None
        for i, tile in enumerate(tiles):
            copies[3 + i].wait()
            one = dot(normed[:, tile], w_ref[tile])
            raw = one if raw is None else raw + one
        full = rms(raw, lgain_ref[...])
        full_ref[...] = full
        latent = full.astype(BF16)
        for (low, high), latent_ref in zip(spans, latent_refs):
            latent_ref[...] = latent[low * rows : high * rows]

    in_turn(0, work, normed_ref, full_ref, *latent_refs)


def next_latent_body(span, hands, rows, n_head, *refs):
    x_ref = refs[0]
    parts = refs[1 : 1 + n_head * len(hands)]
    refs = refs[1 + n_head * len(hands) :]
    gain_ref, w_ref, lgain_ref, before_ref, live_ref = refs[:5]
    state_ref, normed_ref, stored_ref, latent_ref = refs[5:]
    at = slice(span[0] * rows, span[1] * rows)

    def work():
        states = []
        for i, (low, high) in enumerate(hands):
            terms = [p[...] for p in parts[i * n_head : (i + 1) * n_head]]
            states.append(x_ref[low * rows : high * rows].astype(F32) + tree_sum(terms))
        state = jnp.concatenate(states, axis=0)
        state_ref[...] = state
        normed = rms(state, gain_ref[...]).astype(BF16)
        normed_ref[...] = normed
        full = rms(dot(normed, w_ref[...]), lgain_ref[...])
        latent_ref[...] = full.astype(BF16)
        stored_ref[...] = keep_live(full, live_ref[at])

    in_turn(1, work, state_ref, normed_ref, latent_ref)

    @pl.when(place("section") == 0)
    def _():
        stored_ref[...] = keep_live(before_ref[at], live_ref[at])


def wide_dot(a, b):
    extra = 128 - a.shape[0]
    if extra <= 0:
        return dot(a, b)
    padded = jnp.concatenate([a, jnp.zeros((extra, a.shape[1]), a.dtype)], axis=0)
    return dot(padded, b)[: a.shape[0]]


def absorb(scale, query, wk, out_ref):
    for h in range(out_ref.shape[0]):
        cols = slice(h * HD, (h + 1) * HD)
        one = dot(query[:, cols], wk[:, cols], ((1,), (1,)))
        out_ref[h] = (one * scale).astype(BF16)


def query_body(scale, section, normed_ref, wq_ref, wk_ref, out_ref):
    def work():
        query = wide_dot(normed_ref[...], wq_ref[...]).astype(BF16)
        absorb(scale, query, wk_ref, out_ref)

    in_turn(section, work, out_ref)


def attention(spans, own, rows, n_pieces, offset, absorbed_ref, bias_ref, pieces, wv, kv, ctx, attn):
    heads = absorbed_ref.shape[0]
    rank = kv.shape[1]
    block = n_pieces * rows
    for i, (low, high) in enumerate(spans):
        for g in range(low, min(high, own[1])):
            for k in range(n_pieces):
                piece = pieces[i * n_pieces + k]
                kv[pl.ds(g * block + k * rows, rows), :] = piece[pl.ds((g - low) * rows, rows), :]
    low, high = own
    causal = bias_ref[:, bias_ref.shape[1] - block :]
    for g in range(low, high):
        keys = kv[: (g + 1) * block, :]
        at = g * rows - offset
        absorbed = absorbed_ref[:, at : at + rows, :].reshape(heads * rows, rank)
        scores = dot(absorbed, keys, ((1,), (1,))).reshape(heads, rows, (g + 1) * block)
        bias = jnp.concatenate([bias_ref[:, : g * block], causal], axis=1) if g else causal
        scores = scores + bias[None]
        weights = jnp.exp(scores - jnp.max(scores, axis=2, keepdims=True))
        total = jnp.sum(weights, axis=2, keepdims=True).reshape(heads * rows, 1)
        rounded = weights.astype(BF16).reshape(heads * rows, (g + 1) * block)
        context = (dot(rounded, keys) * (1.0 / total)).astype(BF16)
        at = (g - low) * rows
        ctx[:, at : at + rows, :] = context.reshape(heads, rows, rank)
    for h in range(heads):
        cols = slice(h * HD, (h + 1) * HD)
        attn[:, cols] = dot(ctx[h], wv[:, cols]).astype(BF16)


def attend_body(spans, own, rows, n_pieces, offset, absorbed_ref, bias_ref, *refs):
    n_in = len(spans) * n_pieces
    pieces = refs[:n_in]
    wv, wo, out_ref, kv, ctx, attn = refs[n_in:]

    def work():
        attention(
            spans, own, rows, n_pieces, offset, absorbed_ref, bias_ref, pieces, wv, kv, ctx, attn
        )
        out_ref[...] = dot(attn[...], wo[...]).astype(BF16)

    in_turn(0, work, out_ref)


def attend_last_body(spans, own, rows, n_pieces, offset, n_head, n_sec, absorbed_ref, bias_ref, *refs):
    n_in = len(spans) * n_pieces
    pieces = refs[:n_in]
    wv, wo, state_ref, keep_ref, give_ref = refs[n_in : n_in + 5]
    sends = refs[n_in + 5 : n_in + 4 + n_head]
    kv, ctx, attn, total = refs[n_in + 4 + n_head :]

    def work():
        attention(
            spans, own, rows, n_pieces, offset, absorbed_ref, bias_ref, pieces, wv, kv, ctx, attn
        )
        total[...] = dot(attn[...], wo[...])
        low, high = own
        share = rows // n_head
        width = total.shape[1]
        part = width // n_sec
        head = place("head")
        for g in range(high - low):
            to = slice(g * share, (g + 1) * share)

            def at(h):
                return pl.ds(pl.multiple_of(g * rows + h * share, share), share)

            mine = state_ref[at(head), :] + total[at(head), :]
            give_ref[to] = mine[:, : width - part].astype(BF16)
            keep_ref[to] = mine[:, width - part :]
            for k in range(1, n_head):
                sends[k - 1][to] = total[at(jnp.bitwise_xor(head, k)), :].astype(BF16)

    in_turn(n_sec - 1, work, keep_ref, give_ref, *sends)


def final_body(spans, rows, n_head, n_sec, final_ref, *refs):
    out_ref = refs[-1]
    per = 2 + 2 * (n_head - 1)
    share = rows // n_head
    part = out_ref.shape[2]
    last = jnp.broadcast_to(place("section"), (share, part)) == n_sec - 1
    for i, (low, high) in enumerate(spans):
        keep, given = refs[i * per : i * per + 2]
        came = refs[i * per + 2 : i * per + 1 + n_head]
        relay = refs[i * per + 1 + n_head : (i + 1) * per]
        for g in range(low, high):
            at = slice((g - low) * share, (g - low + 1) * share)
            here = keep[at]
            there = given[at].astype(F32)
            for k in range(n_head - 1):
                here = here + relay[k][at, (n_sec - 1) * part :].astype(F32)
                there = there + came[k][at, :part].astype(F32)
            live = final_ref[g * share : (g + 1) * share]
            out_ref[g] = keep_live(jnp.where(last, here, there), live)


def in_hbm(value):
    return pltpu.with_memory_space_constraint(value, pltpu.HBM)


def params(limit):
    return pltpu.CompilerParams(vmem_limit_bytes=limit * MIB)


def plan(groups):
    cut = max(1, groups - 1)
    two = [(0, cut), (cut, groups)] if cut < groups else [(0, groups)]
    each = [(g, g + 1) for g in range(groups)]
    return two, each, two


def array(dtype, *shape):
    return jax.ShapeDtypeStruct(shape, dtype)


def cost(flops, moved, exps=0):
    return pl.CostEstimate(flops=flops, bytes_accessed=moved, transcendentals=exps)


def after(value, *others):
    return lax.optimization_barrier((value, *others))[0]


def shards(hidden, lengths, attn_gain, w_query, w_latent, latent_gain, w_key, w_value, w_out):
    n_seq = lax.axis_size("seq")
    n_sec = lax.axis_size("section")
    n_head = lax.axis_size("head")
    assert n_sec == 2
    sizes = (n_seq, n_sec, n_head)
    groups, rows, width = hidden.shape
    rank = w_latent.shape[2]
    heads = w_key.shape[2] // HD
    total_rows = groups * rows
    share = rows // n_head
    part_width = width // n_sec
    x = hidden.reshape(total_rows, width)
    wl, wq, wk, wv, wo = w_latent[0], w_query[0], w_key[0], w_value[0], w_out[0]
    cuts = 4
    firsts, hands, nexts = plan(groups)

    def count(span):
        return (span[1] - span[0]) * rows

    def prepare():
        return pl.pallas_call(
            functools.partial(prepare_body, rows, n_seq),
            out_shape=(
                array(F32, rows, (groups + 1) * n_seq * rows),
                array(F32, total_rows, HD),
                array(F32, groups * share, HD),
            ),
            in_specs=[SMEM],
            out_specs=(VMEM,) * 3,
            compiler_params=params(8),
            cost_estimate=cost(6 * 10**9, 1 << 20),
            name="prepare",
        )(in_hbm(lengths))

    def first_latent():
        out = pl.pallas_call(
            functools.partial(first_latent_body, firsts, rows, cuts),
            out_shape=(
                array(BF16, total_rows, width),
                array(F32, total_rows, rank),
                *(array(BF16, count(span), rank) for span in firsts),
            ),
            in_specs=[HBM] * 4,
            out_specs=(VMEM,) * (2 + len(firsts)),
            scratch_shapes=[
                pltpu.VMEM((total_rows, width), BF16),
                pltpu.VMEM((1, width), F32),
                pltpu.VMEM((1, rank), F32),
                pltpu.VMEM((width, rank), BF16),
                pltpu.SemaphoreType.DMA((3 + cuts,)),
            ],
            compiler_params=params(12),
            name="first_latent",
        )(*(in_hbm(value) for value in (x, attn_gain, wl, latent_gain)))
        return out[0], out[1], list(out[2:])

    def next_latent(i, parts, before):
        span = nexts[i]
        size = count(span)
        inside = [hand for hand in hands if span[0] <= hand[0] < span[1]]
        return pl.pallas_call(
            functools.partial(next_latent_body, span, inside, rows, n_head),
            out_shape=(
                array(F32, size, width),
                array(BF16, size, width),
                array(F32, size, rank),
                array(BF16, size, rank),
            ),
            in_specs=[VMEM] * (6 + len(parts)),
            out_specs=(VMEM,) * 4,
            compiler_params=params(8),
            cost_estimate=cost(2 * size * width * rank, 2 * width * (rank + 2 * size)),
        )(x, *parts, attn_gain, wl, latent_gain, before, live)

    def project(section, normed):
        size = normed.shape[0]
        return pl.pallas_call(
            functools.partial(query_body, 1.0 / HD**0.5, section),
            out_shape=array(BF16, heads, size, rank),
            in_specs=[VMEM] * 3,
            out_specs=VMEM,
            compiler_params=params(8),
            cost_estimate=cost(
                2 * size * heads * HD * (width + rank), 2 * heads * HD * (width + rank + size)
            ),
        )(normed, wq, wk)

    def attend(name, own, absorbed, offset, spans, pieces, state=None):
        high = own[1]
        size = count(own)
        which = [span for span in spans if span[0] < high]
        flat = [piece for of_span in pieces[: len(which)] for piece in of_span]
        scratch = [
            pltpu.VMEM((high * n_seq * rows, rank), BF16),
            pltpu.VMEM((heads, size, rank), BF16),
            pltpu.VMEM((size, heads * HD), BF16),
        ]
        common = dict(
            compiler_params=params(20),
            cost_estimate=cost(
                4 * heads * size * high * n_seq * rows * rank,
                2 * heads * HD * (width + rank),
                heads * size * high * n_seq * rows,
            ),
            name=name,
        )
        if state is None:
            return pl.pallas_call(
                functools.partial(attend_body, which, own, rows, n_seq, offset),
                out_shape=array(BF16, size, width),
                in_specs=[VMEM] * (4 + len(flat)),
                out_specs=VMEM,
                scratch_shapes=scratch,
                **common,
            )(absorbed, bias, *flat, wv, wo)
        small = size // n_head
        return pl.pallas_call(
            functools.partial(attend_last_body, which, own, rows, n_seq, offset, n_head, n_sec),
            out_shape=(
                array(F32, small, part_width),
                array(BF16, small, width - part_width),
                *(array(BF16, small, width) for _ in range(n_head - 1)),
            ),
            in_specs=[VMEM] * (5 + len(flat)),
            out_specs=(VMEM,) * (1 + n_head),
            scratch_shapes=scratch + [pltpu.VMEM((size, width), F32)],
            **common,
        )(absorbed, bias, *flat, wv, wo, state)

    def swap(value):
        return permute(value, sizes, lambda s, c, h: (s, 1 - c, h))

    def cross(value, source, k):
        return permute(
            value, sizes, lambda s, c, h: (s, 1 - c, h ^ k) if c == source else (s, 1 - c, h)
        )

    def gather(latent, tick):
        there = swap(latent)
        return [latent] + [
            permute(
                there, sizes, lambda s, c, h, k=k: (s, 1 - c, h) if c == tick else (s ^ k, tick, h)
            )
            for k in range(1, n_seq)
        ]

    def hand_on(partial):
        return [swap(partial)] + [cross(partial, 0, k) for k in range(1, n_head)]

    normed, full, latents = first_latent()
    pieces = [gather(latent, 0) for latent in latents]
    bias, live, final_live = prepare()
    absorbed = project(0, normed)
    parts = [
        hand_on(attend(f"attend_0_{i}", own, absorbed, 0, firsts, pieces))
        for i, own in enumerate(hands)
    ]
    pieces, queries, states, lives = [], [], [], []
    for i, span in enumerate(nexts):
        part = []
        for hand, one in zip(hands, parts):
            if span[0] <= hand[0] < span[1]:
                part += [after(p, queries[-1]) for p in one] if i else one
        state, normed, stored, latent = next_latent(i, part, full)
        states.append(state)
        lives.append(stored)
        pieces.append(gather(latent, 1))
        queries.append(project(1, normed))
    ends = []
    for i, own in enumerate(nexts):
        keep, give, *sends = attend(
            f"attend_1_{i}", own, queries[i], own[0] * rows, nexts, pieces, states[i]
        )
        given = swap(give)
        came = [cross(sends[k - 1], 1, k) for k in range(1, n_head)]
        relay = [swap(one) for one in came]
        ends += [keep, given, *came, *relay]
    final = pl.pallas_call(
        functools.partial(final_body, nexts, rows, n_head, n_sec),
        out_shape=array(F32, groups, share, part_width),
        in_specs=[VMEM] * (1 + len(ends)),
        out_specs=VMEM,
        compiler_params=params(12),
        name="final",
    )(final_live, *ends)
    stored = jnp.concatenate(lives, 0).reshape(1, groups, rows, rank)
    return (final, stored)


def solution(mesh):
    return jax.shard_map(
        shards,
        mesh=mesh,
        in_specs=(
            P("rep", "seq", None),
            P("rep"),
            P("section", None),
            P("section", None, "head"),
            P("section", None, None),
            P("section", None),
            P("section", None, "head"),
            P("section", None, "head"),
            P("section", "head", None),
        ),
        out_specs=(P("rep", ("seq", "head"), "section"), P("section", "rep", "seq", None)),
        check_vma=False,
    )
```

```python
import functools

import jax
import jax.numpy as jnp
from jax import lax
from jax.experimental import pallas as pl
from jax.experimental.pallas import tpu as pltpu
from jax.sharding import PartitionSpec as P


HD = 128
AXES = ("seq", "section", "head")
F32 = jnp.float32
BF16 = jnp.bfloat16
VMEM = pl.BlockSpec(memory_space=pltpu.VMEM)
HBM = pl.BlockSpec(memory_space=pltpu.HBM)
SMEM = pl.BlockSpec(memory_space=pltpu.SMEM)
MIB = 1 << 20


def permute(value, sizes, target):
    pairs = []
    for s in range(sizes[0]):
        for c in range(sizes[1]):
            for h in range(sizes[2]):
                ts, tc, th = target(s, c, h)
                at = (s * sizes[1] + c) * sizes[2] + h
                to = (ts * sizes[1] + tc) * sizes[2] + th
                pairs.append((at, to))
    return lax.ppermute(value, AXES, pairs)


def rms(values, gain):
    mean_sq = jnp.mean(values * values, axis=-1, keepdims=True)
    return values * lax.rsqrt(mean_sq + 1e-06) * gain


def dot(a, b, dims=((1,), (0,))):
    return lax.dot_general(a, b, (dims, ((), ())), preferred_element_type=F32)


def tree_sum(terms):
    terms = [t.astype(F32) for t in terms]
    while len(terms) > 1:
        terms = [sum(terms[i : i + 2]) for i in range(0, len(terms), 2)]
    return terms[0]


def place(axis):
    return lax.axis_index(axis).astype(jnp.int32)


def in_turn(section, work, *outs):
    pl.when(place("section") == section)(work)

    @pl.when(place("section") != section)
    def _():
        for out in outs:
            out[...] = jnp.zeros_like(out)


def alive(at, length):
    return jnp.where(at < length, 1.0, 0.0)


def prepare_body(rows, n_pieces, lengths_ref, bias_ref, live_ref, final_ref):
    groups = lengths_ref.shape[0]
    block = n_pieces * rows
    me = place("seq")
    col = lax.broadcasted_iota(jnp.int32, (rows, block), 1)
    row = lax.broadcasted_iota(jnp.int32, (rows, block), 0)
    key_pos = jnp.bitwise_xor(me, col // rows) * rows + col % rows
    for g in range(groups):
        bias_ref[:, g * block : (g + 1) * block] = jnp.where(key_pos < lengths_ref[g], 0.0, -1e30)
    bias_ref[:, groups * block :] = jnp.where(key_pos <= me * rows + row, 0.0, -1e30)
    share = final_ref.shape[0] // groups
    lanes = live_ref.shape[1]
    at = me * rows + lax.broadcasted_iota(jnp.int32, (rows, lanes), 0)
    shared_at = me * rows + place("head") * share
    shared_at = shared_at + lax.broadcasted_iota(jnp.int32, (share, lanes), 0)
    for g in range(groups):
        live_ref[g * rows : (g + 1) * rows] = alive(at, lengths_ref[g])
        final_ref[g * share : (g + 1) * share] = alive(shared_at, lengths_ref[g])


def keep_live(values, live):
    return jnp.where(live[:, :1] > 0.5, values, 0.0)


def first_latent_body(spans, rows, cuts, *refs):
    x_hbm, gain_hbm, w_hbm, lgain_hbm, normed_ref, full_ref = refs[:6]
    latent_refs = refs[6 : 6 + len(spans)]
    x_ref, gain_ref, lgain_ref, w_ref, sems = refs[6 + len(spans) :]

    def work():
        copies = [
            pltpu.make_async_copy(source, to, sems.at[i])
            for i, (source, to) in enumerate(
                ((x_hbm, x_ref), (gain_hbm, gain_ref), (lgain_hbm, lgain_ref))
            )
        ]
        depth = w_ref.shape[0] // cuts
        tiles = [slice(i * depth, (i + 1) * depth) for i in range(cuts)]
        for i, tile in enumerate(tiles):
            copies.append(pltpu.make_async_copy(w_hbm.at[tile], w_ref.at[tile], sems.at[3 + i]))
        for copy in copies:
            copy.start()
        copies[0].wait()
        copies[1].wait()
        normed = rms(x_ref[...].astype(F32), gain_ref[...]).astype(BF16)
        normed_ref[...] = normed
        copies[2].wait()
        raw = None
        for i, tile in enumerate(tiles):
            copies[3 + i].wait()
            one = dot(normed[:, tile], w_ref[tile])
            raw = one if raw is None else raw + one
        full = rms(raw, lgain_ref[...])
        full_ref[...] = full
        latent = full.astype(BF16)
        for (low, high), latent_ref in zip(spans, latent_refs):
            latent_ref[...] = latent[low * rows : high * rows]

    in_turn(0, work, normed_ref, full_ref, *latent_refs)


def next_latent_body(span, hands, rows, n_head, *refs):
    x_ref = refs[0]
    parts = refs[1 : 1 + n_head * len(hands)]
    refs = refs[1 + n_head * len(hands) :]
    gain_ref, w_ref, lgain_ref, before_ref, live_ref = refs[:5]
    state_ref, normed_ref, stored_ref, latent_ref = refs[5:]
    at = slice(span[0] * rows, span[1] * rows)

    def work():
        states = []
        for i, (low, high) in enumerate(hands):
            terms = [p[...] for p in parts[i * n_head : (i + 1) * n_head]]
            states.append(x_ref[low * rows : high * rows].astype(F32) + tree_sum(terms))
        state = jnp.concatenate(states, axis=0)
        state_ref[...] = state
        normed = rms(state, gain_ref[...]).astype(BF16)
        normed_ref[...] = normed
        full = rms(dot(normed, w_ref[...]), lgain_ref[...])
        latent_ref[...] = full.astype(BF16)
        stored_ref[...] = keep_live(full, live_ref[at])

    in_turn(1, work, state_ref, normed_ref, latent_ref)

    @pl.when(place("section") == 0)
    def _():
        stored_ref[...] = keep_live(before_ref[at], live_ref[at])


def wide_dot(a, b):
    extra = 128 - a.shape[0]
    if extra <= 0:
        return dot(a, b)
    padded = jnp.concatenate([a, jnp.zeros((extra, a.shape[1]), a.dtype)], axis=0)
    return dot(padded, b)[: a.shape[0]]


def absorb(scale, query, wk, out_ref):
    for h in range(out_ref.shape[0]):
        cols = slice(h * HD, (h + 1) * HD)
        one = dot(query[:, cols], wk[:, cols], ((1,), (1,)))
        out_ref[h] = (one * scale).astype(BF16)


def query_body(scale, section, normed_ref, wq_ref, wk_ref, out_ref):
    def work():
        query = wide_dot(normed_ref[...], wq_ref[...]).astype(BF16)
        absorb(scale, query, wk_ref, out_ref)

    in_turn(section, work, out_ref)


def attention(spans, own, rows, n_pieces, offset, absorbed_ref, bias_ref, pieces, wv, kv, ctx, attn):
    heads = absorbed_ref.shape[0]
    rank = kv.shape[1]
    block = n_pieces * rows
    for i, (low, high) in enumerate(spans):
        for g in range(low, min(high, own[1])):
            for k in range(n_pieces):
                piece = pieces[i * n_pieces + k]
                kv[pl.ds(g * block + k * rows, rows), :] = piece[pl.ds((g - low) * rows, rows), :]
    low, high = own
    causal = bias_ref[:, bias_ref.shape[1] - block :]
    for g in range(low, high):
        keys = kv[: (g + 1) * block, :]
        at = g * rows - offset
        absorbed = absorbed_ref[:, at : at + rows, :].reshape(heads * rows, rank)
        scores = dot(absorbed, keys, ((1,), (1,))).reshape(heads, rows, (g + 1) * block)
        bias = jnp.concatenate([bias_ref[:, : g * block], causal], axis=1) if g else causal
        scores = scores + bias[None]
        weights = jnp.exp(scores - jnp.max(scores, axis=2, keepdims=True))
        total = jnp.sum(weights, axis=2, keepdims=True).reshape(heads * rows, 1)
        rounded = weights.astype(BF16).reshape(heads * rows, (g + 1) * block)
        context = (dot(rounded, keys) * (1.0 / total)).astype(BF16)
        at = (g - low) * rows
        ctx[:, at : at + rows, :] = context.reshape(heads, rows, rank)
    for h in range(heads):
        cols = slice(h * HD, (h + 1) * HD)
        attn[:, cols] = dot(ctx[h], wv[:, cols]).astype(BF16)


def attend_body(spans, own, rows, n_pieces, offset, absorbed_ref, bias_ref, *refs):
    n_in = len(spans) * n_pieces
    pieces = refs[:n_in]
    wv, wo, out_ref, kv, ctx, attn = refs[n_in:]

    def work():
        attention(
            spans, own, rows, n_pieces, offset, absorbed_ref, bias_ref, pieces, wv, kv, ctx, attn
        )
        out_ref[...] = dot(attn[...], wo[...]).astype(BF16)

    in_turn(0, work, out_ref)


def attend_last_body(spans, own, rows, n_pieces, offset, n_head, n_sec, absorbed_ref, bias_ref, *refs):
    n_in = len(spans) * n_pieces
    pieces = refs[:n_in]
    wv, wo, state_ref, keep_ref, give_ref = refs[n_in : n_in + 5]
    sends = refs[n_in + 5 : n_in + 4 + n_head]
    kv, ctx, attn, total = refs[n_in + 4 + n_head :]

    def work():
        attention(
            spans, own, rows, n_pieces, offset, absorbed_ref, bias_ref, pieces, wv, kv, ctx, attn
        )
        total[...] = dot(attn[...], wo[...])
        low, high = own
        share = rows // n_head
        width = total.shape[1]
        part = width // n_sec
        head = place("head")
        for g in range(high - low):
            to = slice(g * share, (g + 1) * share)

            def at(h):
                return pl.ds(pl.multiple_of(g * rows + h * share, share), share)

            mine = state_ref[at(head), :] + total[at(head), :]
            give_ref[to] = mine[:, : width - part].astype(BF16)
            keep_ref[to] = mine[:, width - part :]
            for k in range(1, n_head):
                sends[k - 1][to] = total[at(jnp.bitwise_xor(head, k)), :].astype(BF16)

    in_turn(n_sec - 1, work, keep_ref, give_ref, *sends)


def final_body(spans, rows, n_head, n_sec, final_ref, *refs):
    out_ref = refs[-1]
    per = 2 + 2 * (n_head - 1)
    share = rows // n_head
    part = out_ref.shape[2]
    last = jnp.broadcast_to(place("section"), (share, part)) == n_sec - 1
    for i, (low, high) in enumerate(spans):
        keep, given = refs[i * per : i * per + 2]
        came = refs[i * per + 2 : i * per + 1 + n_head]
        relay = refs[i * per + 1 + n_head : (i + 1) * per]
        for g in range(low, high):
            at = slice((g - low) * share, (g - low + 1) * share)
            here = keep[at]
            there = given[at].astype(F32)
            for k in range(n_head - 1):
                here = here + relay[k][at, (n_sec - 1) * part :].astype(F32)
                there = there + came[k][at, :part].astype(F32)
            live = final_ref[g * share : (g + 1) * share]
            out_ref[g] = keep_live(jnp.where(last, here, there), live)


def in_hbm(value):
    return pltpu.with_memory_space_constraint(value, pltpu.HBM)


def params(limit):
    return pltpu.CompilerParams(vmem_limit_bytes=limit * MIB)


def plan(groups):
    cut = max(1, groups - 1)
    two = [(0, cut), (cut, groups)] if cut < groups else [(0, groups)]
    each = [(g, g + 1) for g in range(groups)]
    return two, each, two


def array(dtype, *shape):
    return jax.ShapeDtypeStruct(shape, dtype)


def cost(flops, moved, exps=0):
    return pl.CostEstimate(flops=flops, bytes_accessed=moved, transcendentals=exps)


def after(value, *others):
    return lax.optimization_barrier((value, *others))[0]


def shards(hidden, lengths, attn_gain, w_query, w_latent, latent_gain, w_key, w_value, w_out):
    n_seq = lax.axis_size("seq")
    n_sec = lax.axis_size("section")
    n_head = lax.axis_size("head")
    assert n_sec == 2
    sizes = (n_seq, n_sec, n_head)
    groups, rows, width = hidden.shape
    rank = w_latent.shape[2]
    heads = w_key.shape[2] // HD
    total_rows = groups * rows
    share = rows // n_head
    part_width = width // n_sec
    x = hidden.reshape(total_rows, width)
    wl, wq, wk, wv, wo = w_latent[0], w_query[0], w_key[0], w_value[0], w_out[0]
    cuts = 4
    firsts, hands, nexts = plan(groups)

    def count(span):
        return (span[1] - span[0]) * rows

    def prepare():
        return pl.pallas_call(
            functools.partial(prepare_body, rows, n_seq),
            out_shape=(
                array(F32, rows, (groups + 1) * n_seq * rows),
                array(F32, total_rows, HD),
                array(F32, groups * share, HD),
            ),
            in_specs=[SMEM],
            out_specs=(VMEM,) * 3,
            compiler_params=params(8),
            cost_estimate=cost(6 * 10**9, 1 << 20),
            name="prepare",
        )(in_hbm(lengths))

    def first_latent():
        out = pl.pallas_call(
            functools.partial(first_latent_body, firsts, rows, cuts),
            out_shape=(
                array(BF16, total_rows, width),
                array(F32, total_rows, rank),
                *(array(BF16, count(span), rank) for span in firsts),
            ),
            in_specs=[HBM] * 4,
            out_specs=(VMEM,) * (2 + len(firsts)),
            scratch_shapes=[
                pltpu.VMEM((total_rows, width), BF16),
                pltpu.VMEM((1, width), F32),
                pltpu.VMEM((1, rank), F32),
                pltpu.VMEM((width, rank), BF16),
                pltpu.SemaphoreType.DMA((3 + cuts,)),
            ],
            compiler_params=params(12),
            name="first_latent",
        )(*(in_hbm(value) for value in (x, attn_gain, wl, latent_gain)))
        return out[0], out[1], list(out[2:])

    def next_latent(i, parts, before):
        span = nexts[i]
        size = count(span)
        inside = [hand for hand in hands if span[0] <= hand[0] < span[1]]
        return pl.pallas_call(
            functools.partial(next_latent_body, span, inside, rows, n_head),
            out_shape=(
                array(F32, size, width),
                array(BF16, size, width),
                array(F32, size, rank),
                array(BF16, size, rank),
            ),
            in_specs=[VMEM] * (6 + len(parts)),
            out_specs=(VMEM,) * 4,
            compiler_params=params(8),
            cost_estimate=cost(2 * size * width * rank, 2 * width * (rank + 2 * size)),
        )(x, *parts, attn_gain, wl, latent_gain, before, live)

    def project(section, normed):
        size = normed.shape[0]
        return pl.pallas_call(
            functools.partial(query_body, 1.0 / HD**0.5, section),
            out_shape=array(BF16, heads, size, rank),
            in_specs=[VMEM] * 3,
            out_specs=VMEM,
            compiler_params=params(8),
            cost_estimate=cost(
                2 * size * heads * HD * (width + rank), 2 * heads * HD * (width + rank + size)
            ),
        )(normed, wq, wk)

    def attend(name, own, absorbed, offset, spans, pieces, state=None):
        high = own[1]
        size = count(own)
        which = [span for span in spans if span[0] < high]
        flat = [piece for of_span in pieces[: len(which)] for piece in of_span]
        scratch = [
            pltpu.VMEM((high * n_seq * rows, rank), BF16),
            pltpu.VMEM((heads, size, rank), BF16),
            pltpu.VMEM((size, heads * HD), BF16),
        ]
        common = dict(
            compiler_params=params(20),
            cost_estimate=cost(
                4 * heads * size * high * n_seq * rows * rank,
                2 * heads * HD * (width + rank),
                heads * size * high * n_seq * rows,
            ),
            name=name,
        )
        if state is None:
            return pl.pallas_call(
                functools.partial(attend_body, which, own, rows, n_seq, offset),
                out_shape=array(BF16, size, width),
                in_specs=[VMEM] * (4 + len(flat)),
                out_specs=VMEM,
                scratch_shapes=scratch,
                **common,
            )(absorbed, bias, *flat, wv, wo)
        small = size // n_head
        return pl.pallas_call(
            functools.partial(attend_last_body, which, own, rows, n_seq, offset, n_head, n_sec),
            out_shape=(
                array(F32, small, part_width),
                array(BF16, small, width - part_width),
                *(array(BF16, small, width) for _ in range(n_head - 1)),
            ),
            in_specs=[VMEM] * (5 + len(flat)),
            out_specs=(VMEM,) * (1 + n_head),
            scratch_shapes=scratch + [pltpu.VMEM((size, width), F32)],
            **common,
        )(absorbed, bias, *flat, wv, wo, state)

    def swap(value):
        return permute(value, sizes, lambda s, c, h: (s, 1 - c, h))

    def cross(value, source, k):
        return permute(
            value, sizes, lambda s, c, h: (s, 1 - c, h ^ k) if c == source else (s, 1 - c, h)
        )

    def flip(value, source, k):
        return permute(
            value, sizes, lambda s, c, h: (s ^ k, 1 - c, h) if c == source else (s, 1 - c, h)
        )

    def gather(latent, tick):
        if n_seq != 4:
            there = swap(latent)
            return [latent] + [flip(there, 1 - tick, k) for k in range(1, n_seq)]
        far = flip(latent, tick, 2)
        side = flip(latent, tick, 1)
        turned = flip(far, 1 - tick, 1)
        return [latent, swap(side), swap(far), turned]

    def hand_on(partial):
        return [swap(partial)] + [cross(partial, 0, k) for k in range(1, n_head)]

    normed, full, latents = first_latent()
    pieces = [gather(latent, 0) for latent in latents]
    bias, live, final_live = prepare()
    absorbed = project(0, normed)
    parts = [
        hand_on(attend(f"attend_0_{i}", own, absorbed, 0, firsts, pieces))
        for i, own in enumerate(hands)
    ]
    pieces, queries, states, lives = [], [], [], []
    for i, span in enumerate(nexts):
        part = []
        for hand, one in zip(hands, parts):
            if span[0] <= hand[0] < span[1]:
                part += [after(p, queries[-1]) for p in one] if i else one
        state, normed, stored, latent = next_latent(i, part, full)
        states.append(state)
        lives.append(stored)
        pieces.append(gather(latent, 1))
        queries.append(project(1, normed))
    ends = []
    for i, own in enumerate(nexts):
        keep, give, *sends = attend(
            f"attend_1_{i}", own, queries[i], own[0] * rows, nexts, pieces, states[i]
        )
        given = swap(give)
        came = [cross(sends[k - 1], 1, k) for k in range(1, n_head)]
        relay = [swap(one) for one in came]
        ends += [keep, given, *came, *relay]
    final = pl.pallas_call(
        functools.partial(final_body, nexts, rows, n_head, n_sec),
        out_shape=array(F32, groups, share, part_width),
        in_specs=[VMEM] * (1 + len(ends)),
        out_specs=VMEM,
        compiler_params=params(12),
        name="final",
    )(final_live, *ends)
    stored = jnp.concatenate(lives, 0).reshape(1, groups, rows, rank)
    return (final, stored)


def solution(mesh):
    return jax.shard_map(
        shards,
        mesh=mesh,
        in_specs=(
            P("rep", "seq", None),
            P("rep"),
            P("section", None),
            P("section", None, "head"),
            P("section", None, None),
            P("section", None),
            P("section", None, "head"),
            P("section", None, "head"),
            P("section", "head", None),
        ),
        out_specs=(P("rep", ("seq", "head"), "section"), P("section", "rep", "seq", None)),
        check_vma=False,
    )
```

```python
import functools

import jax
import jax.numpy as jnp
from jax import lax
from jax.experimental import pallas as pl
from jax.experimental.pallas import tpu as pltpu
from jax.sharding import PartitionSpec as P


HD = 128
AXES = ("seq", "section", "head")
F32 = jnp.float32
BF16 = jnp.bfloat16
VMEM = pl.BlockSpec(memory_space=pltpu.VMEM)
HBM = pl.BlockSpec(memory_space=pltpu.HBM)
SMEM = pl.BlockSpec(memory_space=pltpu.SMEM)
MIB = 1 << 20


def permute(value, sizes, target):
    pairs = []
    for s in range(sizes[0]):
        for c in range(sizes[1]):
            for h in range(sizes[2]):
                ts, tc, th = target(s, c, h)
                at = (s * sizes[1] + c) * sizes[2] + h
                to = (ts * sizes[1] + tc) * sizes[2] + th
                pairs.append((at, to))
    return lax.ppermute(value, AXES, pairs)


def rms(values, gain):
    mean_sq = jnp.mean(values * values, axis=-1, keepdims=True)
    return values * lax.rsqrt(mean_sq + 1e-06) * gain


def dot(a, b, dims=((1,), (0,))):
    return lax.dot_general(a, b, (dims, ((), ())), preferred_element_type=F32)


def tree_sum(terms):
    terms = [t.astype(F32) for t in terms]
    while len(terms) > 1:
        terms = [sum(terms[i : i + 2]) for i in range(0, len(terms), 2)]
    return terms[0]


def place(axis):
    return lax.axis_index(axis).astype(jnp.int32)


def in_turn(section, work, *outs):
    pl.when(place("section") == section)(work)

    @pl.when(place("section") != section)
    def _():
        for out in outs:
            out[...] = jnp.zeros_like(out)


def alive(at, length):
    return jnp.where(at < length, 1.0, 0.0)


def prepare_body(rows, n_pieces, lengths_ref, bias_ref, live_ref, final_ref):
    groups = lengths_ref.shape[0]
    block = n_pieces * rows
    me = place("seq")
    col = lax.broadcasted_iota(jnp.int32, (rows, block), 1)
    row = lax.broadcasted_iota(jnp.int32, (rows, block), 0)
    key_pos = jnp.bitwise_xor(me, col // rows) * rows + col % rows
    for g in range(groups):
        bias_ref[:, g * block : (g + 1) * block] = jnp.where(key_pos < lengths_ref[g], 0.0, -1e30)
    bias_ref[:, groups * block :] = jnp.where(key_pos <= me * rows + row, 0.0, -1e30)
    share = final_ref.shape[0] // groups
    lanes = live_ref.shape[1]
    at = me * rows + lax.broadcasted_iota(jnp.int32, (rows, lanes), 0)
    shared_at = me * rows + place("head") * share
    shared_at = shared_at + lax.broadcasted_iota(jnp.int32, (share, lanes), 0)
    for g in range(groups):
        live_ref[g * rows : (g + 1) * rows] = alive(at, lengths_ref[g])
        final_ref[g * share : (g + 1) * share] = alive(shared_at, lengths_ref[g])


def keep_live(values, live):
    return jnp.where(live[:, :1] > 0.5, values, 0.0)


def first_latent_body(spans, rows, cuts, *refs):
    x_hbm, gain_hbm, w_hbm, lgain_hbm, normed_ref, full_ref = refs[:6]
    latent_refs = refs[6 : 6 + len(spans)]
    x_ref, gain_ref, lgain_ref, w_ref, sems = refs[6 + len(spans) :]

    def work():
        copies = [
            pltpu.make_async_copy(source, to, sems.at[i])
            for i, (source, to) in enumerate(
                ((x_hbm, x_ref), (gain_hbm, gain_ref), (lgain_hbm, lgain_ref))
            )
        ]
        depth = w_ref.shape[0] // cuts
        tiles = [slice(i * depth, (i + 1) * depth) for i in range(cuts)]
        for i, tile in enumerate(tiles):
            copies.append(pltpu.make_async_copy(w_hbm.at[tile], w_ref.at[tile], sems.at[3 + i]))
        for copy in copies:
            copy.start()
        copies[0].wait()
        copies[1].wait()
        normed = rms(x_ref[...].astype(F32), gain_ref[...]).astype(BF16)
        normed_ref[...] = normed
        copies[2].wait()
        raw = None
        for i, tile in enumerate(tiles):
            copies[3 + i].wait()
            one = dot(normed[:, tile], w_ref[tile])
            raw = one if raw is None else raw + one
        full = rms(raw, lgain_ref[...])
        full_ref[...] = full
        latent = full.astype(BF16)
        for (low, high), latent_ref in zip(spans, latent_refs):
            latent_ref[...] = latent[low * rows : high * rows]

    in_turn(0, work, normed_ref, full_ref, *latent_refs)


def next_latent_body(span, hands, rows, n_head, *refs):
    x_ref = refs[0]
    parts = refs[1 : 1 + n_head * len(hands)]
    refs = refs[1 + n_head * len(hands) :]
    gain_ref, w_ref, lgain_ref, before_ref, live_ref = refs[:5]
    state_ref, normed_ref, stored_ref, latent_ref = refs[5:]
    at = slice(span[0] * rows, span[1] * rows)

    def work():
        states = []
        for i, (low, high) in enumerate(hands):
            terms = [p[...] for p in parts[i * n_head : (i + 1) * n_head]]
            states.append(x_ref[low * rows : high * rows].astype(F32) + tree_sum(terms))
        state = jnp.concatenate(states, axis=0)
        state_ref[...] = state
        normed = rms(state, gain_ref[...]).astype(BF16)
        normed_ref[...] = normed
        full = rms(dot(normed, w_ref[...]), lgain_ref[...])
        latent_ref[...] = full.astype(BF16)
        stored_ref[...] = keep_live(full, live_ref[at])

    in_turn(1, work, state_ref, normed_ref, latent_ref)

    @pl.when(place("section") == 0)
    def _():
        stored_ref[...] = keep_live(before_ref[at], live_ref[at])


def wide_dot(a, b):
    extra = 128 - a.shape[0]
    if extra <= 0:
        return dot(a, b)
    padded = jnp.concatenate([a, jnp.zeros((extra, a.shape[1]), a.dtype)], axis=0)
    return dot(padded, b)[: a.shape[0]]


def absorb(scale, query, wk, out_ref):
    for h in range(out_ref.shape[0]):
        cols = slice(h * HD, (h + 1) * HD)
        one = dot(query[:, cols], wk[:, cols], ((1,), (1,)))
        out_ref[h] = (one * scale).astype(BF16)


def query_body(scale, section, normed_ref, wq_ref, wk_ref, out_ref):
    def work():
        query = wide_dot(normed_ref[...], wq_ref[...]).astype(BF16)
        absorb(scale, query, wk_ref, out_ref)

    in_turn(section, work, out_ref)


def attention(spans, own, rows, n_pieces, offset, absorbed_ref, bias_ref, pieces, wv, kv, ctx, attn):
    heads = absorbed_ref.shape[0]
    rank = kv.shape[1]
    block = n_pieces * rows
    for i, (low, high) in enumerate(spans):
        for g in range(low, min(high, own[1])):
            for k in range(n_pieces):
                piece = pieces[i * n_pieces + k]
                kv[pl.ds(g * block + k * rows, rows), :] = piece[pl.ds((g - low) * rows, rows), :]
    low, high = own
    causal = bias_ref[:, bias_ref.shape[1] - block :]
    for g in range(low, high):
        keys = kv[: (g + 1) * block, :]
        at = g * rows - offset
        absorbed = absorbed_ref[:, at : at + rows, :].reshape(heads * rows, rank)
        scores = dot(absorbed, keys, ((1,), (1,))).reshape(heads, rows, (g + 1) * block)
        bias = jnp.concatenate([bias_ref[:, : g * block], causal], axis=1) if g else causal
        scores = scores + bias[None]
        weights = jnp.exp(scores - jnp.max(scores, axis=2, keepdims=True))
        total = jnp.sum(weights, axis=2, keepdims=True).reshape(heads * rows, 1)
        rounded = weights.astype(BF16).reshape(heads * rows, (g + 1) * block)
        context = (dot(rounded, keys) * (1.0 / total)).astype(BF16)
        at = (g - low) * rows
        ctx[:, at : at + rows, :] = context.reshape(heads, rows, rank)
    for h in range(heads):
        cols = slice(h * HD, (h + 1) * HD)
        attn[:, cols] = dot(ctx[h], wv[:, cols]).astype(BF16)


def attend_body(spans, own, rows, n_pieces, offset, absorbed_ref, bias_ref, *refs):
    n_in = len(spans) * n_pieces
    pieces = refs[:n_in]
    wv, wo, out_ref, kv, ctx, attn = refs[n_in:]

    def work():
        attention(
            spans, own, rows, n_pieces, offset, absorbed_ref, bias_ref, pieces, wv, kv, ctx, attn
        )
        out_ref[...] = dot(attn[...], wo[...]).astype(BF16)

    in_turn(0, work, out_ref)


def attend_last_body(spans, own, rows, n_pieces, offset, n_head, n_sec, absorbed_ref, bias_ref, *refs):
    n_in = len(spans) * n_pieces
    pieces = refs[:n_in]
    wv, wo, state_ref, keep_ref, give_ref = refs[n_in : n_in + 5]
    sends = refs[n_in + 5 : n_in + 4 + n_head]
    kv, ctx, attn, total = refs[n_in + 4 + n_head :]

    def work():
        attention(
            spans, own, rows, n_pieces, offset, absorbed_ref, bias_ref, pieces, wv, kv, ctx, attn
        )
        total[...] = dot(attn[...], wo[...])
        low, high = own
        share = rows // n_head
        width = total.shape[1]
        part = width // n_sec
        head = place("head")
        for g in range(high - low):
            to = slice(g * share, (g + 1) * share)

            def at(h):
                return pl.ds(pl.multiple_of(g * rows + h * share, share), share)

            mine = state_ref[at(head), :] + total[at(head), :]
            give_ref[to] = mine[:, : width - part].astype(BF16)
            keep_ref[to] = mine[:, width - part :]
            for k in range(1, n_head):
                sends[k - 1][to] = total[at(jnp.bitwise_xor(head, k)), :].astype(BF16)

    in_turn(n_sec - 1, work, keep_ref, give_ref, *sends)


def final_body(spans, rows, n_head, n_sec, final_ref, *refs):
    out_hbm, held, sems = refs[-3:]
    copies = []
    per = 2 + 2 * (n_head - 1)
    share = rows // n_head
    part = held.shape[2]
    last = jnp.broadcast_to(place("section"), (share, part)) == n_sec - 1
    for i, (low, high) in enumerate(spans):
        keep, given = refs[i * per : i * per + 2]
        came = refs[i * per + 2 : i * per + 1 + n_head]
        relay = refs[i * per + 1 + n_head : (i + 1) * per]
        for g in range(low, high):
            at = slice((g - low) * share, (g - low + 1) * share)
            here = keep[at]
            there = given[at].astype(F32)
            for k in range(n_head - 1):
                here = here + relay[k][at, (n_sec - 1) * part :].astype(F32)
                there = there + came[k][at, :part].astype(F32)
            live = final_ref[g * share : (g + 1) * share]
            held[g] = keep_live(jnp.where(last, here, there), live)
            copies.append(pltpu.make_async_copy(held.at[g], out_hbm.at[g], sems.at[g]))
            copies[-1].start()
    for copy in copies:
        copy.wait()


def in_hbm(value):
    return pltpu.with_memory_space_constraint(value, pltpu.HBM)


def params(limit):
    return pltpu.CompilerParams(vmem_limit_bytes=limit * MIB)


def plan(groups):
    cut = max(1, groups - 1)
    two = [(0, cut), (cut, groups)] if cut < groups else [(0, groups)]
    each = [(g, g + 1) for g in range(groups)]
    return two, each, two


def array(dtype, *shape):
    return jax.ShapeDtypeStruct(shape, dtype)


def cost(flops, moved, exps=0):
    return pl.CostEstimate(flops=flops, bytes_accessed=moved, transcendentals=exps)


def after(value, *others):
    return lax.optimization_barrier((value, *others))[0]


def shards(hidden, lengths, attn_gain, w_query, w_latent, latent_gain, w_key, w_value, w_out):
    n_seq = lax.axis_size("seq")
    n_sec = lax.axis_size("section")
    n_head = lax.axis_size("head")
    assert n_sec == 2
    sizes = (n_seq, n_sec, n_head)
    groups, rows, width = hidden.shape
    rank = w_latent.shape[2]
    heads = w_key.shape[2] // HD
    total_rows = groups * rows
    share = rows // n_head
    part_width = width // n_sec
    x = hidden.reshape(total_rows, width)
    wl, wq, wk, wv, wo = w_latent[0], w_query[0], w_key[0], w_value[0], w_out[0]
    cuts = 4
    firsts, hands, nexts = plan(groups)

    def count(span):
        return (span[1] - span[0]) * rows

    def prepare():
        return pl.pallas_call(
            functools.partial(prepare_body, rows, n_seq),
            out_shape=(
                array(F32, rows, (groups + 1) * n_seq * rows),
                array(F32, total_rows, HD),
                array(F32, groups * share, HD),
            ),
            in_specs=[SMEM],
            out_specs=(VMEM,) * 3,
            compiler_params=params(8),
            cost_estimate=cost(6 * 10**9, 1 << 20),
            name="prepare",
        )(in_hbm(lengths))

    def first_latent():
        out = pl.pallas_call(
            functools.partial(first_latent_body, firsts, rows, cuts),
            out_shape=(
                array(BF16, total_rows, width),
                array(F32, total_rows, rank),
                *(array(BF16, count(span), rank) for span in firsts),
            ),
            in_specs=[HBM] * 4,
            out_specs=(VMEM,) * (2 + len(firsts)),
            scratch_shapes=[
                pltpu.VMEM((total_rows, width), BF16),
                pltpu.VMEM((1, width), F32),
                pltpu.VMEM((1, rank), F32),
                pltpu.VMEM((width, rank), BF16),
                pltpu.SemaphoreType.DMA((3 + cuts,)),
            ],
            compiler_params=params(12),
            name="first_latent",
        )(*(in_hbm(value) for value in (x, attn_gain, wl, latent_gain)))
        return out[0], out[1], list(out[2:])

    def next_latent(i, parts, before):
        span = nexts[i]
        size = count(span)
        inside = [hand for hand in hands if span[0] <= hand[0] < span[1]]
        return pl.pallas_call(
            functools.partial(next_latent_body, span, inside, rows, n_head),
            out_shape=(
                array(F32, size, width),
                array(BF16, size, width),
                array(F32, size, rank),
                array(BF16, size, rank),
            ),
            in_specs=[VMEM] * (6 + len(parts)),
            out_specs=(VMEM,) * 4,
            compiler_params=params(8),
            cost_estimate=cost(2 * size * width * rank, 2 * width * (rank + 2 * size)),
        )(x, *parts, attn_gain, wl, latent_gain, before, live)

    def project(section, normed):
        size = normed.shape[0]
        return pl.pallas_call(
            functools.partial(query_body, 1.0 / HD**0.5, section),
            out_shape=array(BF16, heads, size, rank),
            in_specs=[VMEM] * 3,
            out_specs=VMEM,
            compiler_params=params(8),
            cost_estimate=cost(
                2 * size * heads * HD * (width + rank), 2 * heads * HD * (width + rank + size)
            ),
        )(normed, wq, wk)

    def attend(name, own, absorbed, offset, spans, pieces, state=None):
        high = own[1]
        size = count(own)
        which = [span for span in spans if span[0] < high]
        flat = [piece for of_span in pieces[: len(which)] for piece in of_span]
        scratch = [
            pltpu.VMEM((high * n_seq * rows, rank), BF16),
            pltpu.VMEM((heads, size, rank), BF16),
            pltpu.VMEM((size, heads * HD), BF16),
        ]
        common = dict(
            compiler_params=params(20),
            cost_estimate=cost(
                4 * heads * size * high * n_seq * rows * rank,
                2 * heads * HD * (width + rank),
                heads * size * high * n_seq * rows,
            ),
            name=name,
        )
        if state is None:
            return pl.pallas_call(
                functools.partial(attend_body, which, own, rows, n_seq, offset),
                out_shape=array(BF16, size, width),
                in_specs=[VMEM] * (4 + len(flat)),
                out_specs=VMEM,
                scratch_shapes=scratch,
                **common,
            )(absorbed, bias, *flat, wv, wo)
        small = size // n_head
        return pl.pallas_call(
            functools.partial(attend_last_body, which, own, rows, n_seq, offset, n_head, n_sec),
            out_shape=(
                array(F32, small, part_width),
                array(BF16, small, width - part_width),
                *(array(BF16, small, width) for _ in range(n_head - 1)),
            ),
            in_specs=[VMEM] * (5 + len(flat)),
            out_specs=(VMEM,) * (1 + n_head),
            scratch_shapes=scratch + [pltpu.VMEM((size, width), F32)],
            **common,
        )(absorbed, bias, *flat, wv, wo, state)

    def swap(value):
        return permute(value, sizes, lambda s, c, h: (s, 1 - c, h))

    def cross(value, source, k):
        return permute(
            value, sizes, lambda s, c, h: (s, 1 - c, h ^ k) if c == source else (s, 1 - c, h)
        )

    def flip(value, source, k):
        return permute(
            value, sizes, lambda s, c, h: (s ^ k, 1 - c, h) if c == source else (s, 1 - c, h)
        )

    def gather(latent, tick):
        if n_seq != 4:
            there = swap(latent)
            return [latent] + [flip(there, 1 - tick, k) for k in range(1, n_seq)]
        far = flip(latent, tick, 2)
        side = flip(latent, tick, 1)
        turned = flip(far, 1 - tick, 1)
        return [latent, swap(side), swap(far), turned]

    def hand_on(partial):
        return [swap(partial)] + [cross(partial, 0, k) for k in range(1, n_head)]

    normed, full, latents = first_latent()
    pieces = [gather(latent, 0) for latent in latents]
    bias, live, final_live = prepare()
    absorbed = project(0, normed)
    parts = [
        hand_on(attend(f"attend_0_{i}", own, absorbed, 0, firsts, pieces))
        for i, own in enumerate(hands)
    ]
    pieces, queries, states, lives = [], [], [], []
    for i, span in enumerate(nexts):
        part = []
        for hand, one in zip(hands, parts):
            if span[0] <= hand[0] < span[1]:
                part += [after(p, queries[-1]) for p in one] if i else one
        state, normed, stored, latent = next_latent(i, part, full)
        states.append(state)
        lives.append(stored)
        pieces.append(gather(latent, 1))
        queries.append(project(1, normed))
    ends = []
    for i, own in enumerate(nexts):
        keep, give, *sends = attend(
            f"attend_1_{i}", own, queries[i], own[0] * rows, nexts, pieces, states[i]
        )
        given = swap(give)
        came = [cross(sends[k - 1], 1, k) for k in range(1, n_head)]
        relay = [swap(one) for one in came]
        ends += [keep, given, *came, *relay]
    final = pl.pallas_call(
        functools.partial(final_body, nexts, rows, n_head, n_sec),
        out_shape=array(F32, groups, share, part_width),
        in_specs=[VMEM] * (1 + len(ends)),
        out_specs=HBM,
        scratch_shapes=[
            pltpu.VMEM((groups, share, part_width), F32),
            pltpu.SemaphoreType.DMA((groups,)),
        ],
        compiler_params=params(12),
        name="final",
    )(final_live, *ends)
    stored = jnp.concatenate(lives, 0).reshape(1, groups, rows, rank)
    return (final, stored)


def solution(mesh):
    return jax.shard_map(
        shards,
        mesh=mesh,
        in_specs=(
            P("rep", "seq", None),
            P("rep"),
            P("section", None),
            P("section", None, "head"),
            P("section", None, None),
            P("section", None),
            P("section", None, "head"),
            P("section", None, "head"),
            P("section", "head", None),
        ),
        out_specs=(P("rep", ("seq", "head"), "section"), P("section", "rep", "seq", None)),
        check_vma=False,
    )
```
